128 devices in a mesh: model: 4 (over x), data: 32 (over z, y, core).
Axes of the slice: x: 4, y: 4, z: 4, core: 2. Of those that a mesh axis runs over, the one named last changes fastest.
Arguments:
- local_grads: bfloat16 [32, 24, 589824], P('data', None, 'model')
- master: float32 [24, 589824], P(None, ('model', 'data'))
- moment_one: float32 [24, 589824], P(None, ('model', 'data'))
- moment_two: float32 [24, 589824], P(None, ('model', 'data'))
Outputs:
- output 1: bfloat16 [24, 589824], P(None, 'model')
- output 2: float32 [24, 589824], P(None, ('model', 'data'))
- output 3: float32 [24, 589824], P(None, ('model', 'data'))
- output 4: float32 [24, 589824], P(None, ('model', 'data'))
All inputs are finite; a program needn't handle non-finite values.
Results may differ from the reference program's by a relative error of at most 0.001.
Values are sent between devices in bfloat16 or wider.
A program may use at most 1 GiB of HBM per device.

```python
import jax
import jax.numpy as jnp
from jax import lax

D = 768
LAYERS = 2
DATA = 32
STEP = 4
BLOCKS = 12 * LAYERS
BLOCK_SIZE = D * D
LEARN_RATE = 0.08
BETA_ONE = 0.9
BETA_TWO = 0.999
EPSILON = 1e-6
WEIGHT_DECAY = 0.01
MAX_NORM = 1.0
CORR_ONE = 1.0 - BETA_ONE ** STEP
CORR_TWO = 1.0 - BETA_TWO ** STEP


def tensor_sums(block_values):
    return jnp.stack([block_values[..., 0:3].sum(axis=-1), block_values[..., 3], block_values[..., 4:8].sum(axis=-1), block_values[..., 8:12].sum(axis=-1)], axis=-1)


def spread_tensors(tensor_values):
    lead_shape = tensor_values.shape[:-1]
    pieces = [jnp.broadcast_to(tensor_values[..., tensor_pos:tensor_pos + 1], lead_shape + (block_count,)) for tensor_pos, block_count in enumerate((3, 1, 4, 4))]
    return jnp.concatenate(pieces, axis=-1)


def setup_inputs(seed: int = 0) -> dict:
    key_list = jax.random.split(jax.random.key(seed), 8)
    fan_scale = jnp.concatenate([jnp.full((8,), D ** -0.5, jnp.float32), jnp.full((4,), (4 * D) ** -0.5, jnp.float32)])
    weight_factor = jnp.exp(jax.random.uniform(key_list[0], (LAYERS, 4), jnp.float32, minval=-0.8, maxval=0.8))
    weight_scale = (spread_tensors(weight_factor) * fan_scale).reshape(BLOCKS, 1)
    weight_slope = spread_tensors(jax.random.uniform(key_list[1], (LAYERS, 4), jnp.float32, minval=1.5, maxval=2.5)).reshape(BLOCKS, 1)
    position = jnp.arange(BLOCK_SIZE, dtype=jnp.float32) / BLOCK_SIZE - 0.5
    grad_factor = spread_tensors(jnp.exp(jax.random.uniform(key_list[2], (LAYERS, 4), jnp.float32, minval=-1.0, maxval=1.0))).reshape(BLOCKS, 1)
    grad_sigma = grad_factor * (3.0 * MAX_NORM) / jnp.sqrt(BLOCK_SIZE * jnp.sum(grad_factor * grad_factor))
    unit_scale = grad_sigma / jnp.sqrt(2.0)
    shared = jax.random.normal(key_list[3], (BLOCKS, BLOCK_SIZE), jnp.float32)

    def one_replica(replica):
        replica_noise = jax.random.normal(jax.random.fold_in(key_list[4], replica), (BLOCKS, BLOCK_SIZE), jnp.float32)
        return (unit_scale * (shared + DATA ** 0.5 * replica_noise)).astype(jnp.bfloat16)

    local_grads = lax.map(one_replica, jnp.arange(DATA))
    step_sigma = grad_sigma / 3.0
    master = weight_scale * jnp.exp(weight_slope * position) * jax.random.normal(key_list[5], (BLOCKS, BLOCK_SIZE), jnp.float32)
    moment_one = 0.1 * step_sigma * jax.random.normal(key_list[6], (BLOCKS, BLOCK_SIZE), jnp.float32)
    moment_two = 0.003 * step_sigma * step_sigma * jax.random.uniform(key_list[7], (BLOCKS, BLOCK_SIZE), jnp.float32, minval=0.5, maxval=1.5)
    return {'local_grads': local_grads, 'master': master, 'moment_one': moment_one, 'moment_two': moment_two}


def reference(local_grads, master, moment_one, moment_two):
    grad_mean = jnp.sum(local_grads, axis=0, dtype=jnp.float32) / DATA
    clip_scale = jnp.minimum(1.0, MAX_NORM / jnp.sqrt(jnp.sum(grad_mean * grad_mean)))
    scaled = clip_scale * grad_mean
    new_one = BETA_ONE * moment_one + (1.0 - BETA_ONE) * scaled
    new_two = BETA_TWO * moment_two + (1.0 - BETA_TWO) * scaled * scaled
    direction = (new_one / CORR_ONE) / (jnp.sqrt(new_two / CORR_TWO) + EPSILON) + WEIGHT_DECAY * master
    norm_sq = jnp.stack([jnp.sum(master * master, axis=1), jnp.sum(direction * direction, axis=1)])
    tensor_norms = jnp.sqrt(tensor_sums(norm_sq.reshape(2, LAYERS, 12)))
    block_ratio = spread_tensors(tensor_norms[0] / tensor_norms[1]).reshape(BLOCKS, 1)
    new_master = master - LEARN_RATE * block_ratio * direction
    return new_master.astype(jnp.bfloat16), new_master, new_one, new_two
```

```python
import functools

import jax
import jax.numpy as jnp
from jax import lax
from jax.experimental import pallas as pl
from jax.experimental.pallas import tpu as pltpu
from jax.sharding import PartitionSpec as P

STEP = 4
LEARN_RATE = 0.08
BETA_ONE = 0.9
BETA_TWO = 0.999
EPSILON = 1e-6
WEIGHT_DECAY = 0.01
MAX_NORM = 1.0
CORR_ONE = 1.0 - BETA_ONE ** STEP
CORR_TWO = 1.0 - BETA_TWO ** STEP

MESH = pl.DeviceIdType.MESH
TILES = 3
SLAB = 4608
HALF = SLAB // 2
STEP_COLS = 768
REPLICAS = 32
PLUS_SET = (2, 0)
MINUS_SET = (3, 1)
SUM_ROUNDS = (
    tuple((0, 0, k, 0) for k in (1, 2, 3)),
    tuple((0, k, 0, 0) for k in (1, 2, 3)),
    tuple((k, 0, 0, e) for k in (0, 1, 2, 3) for e in (0, 1) if (k, e) != (0, 0)),
)
SLOTS = max(len(group) for group in SUM_ROUNDS)
COPIES = 120
LOADS = 18


def lamb_kernel(grads, master_in, one_in, two_in, params, master_out, one_out, two_out, own_raw, pair_raw, relay_raw, early, late, fin, sums, mid, end, master, one, two, grad_sum, direction, tiles, slots, send_sem, recv_sem, load_sem):
    x, data = lax.axis_index('model'), lax.axis_index('data')
    core, y, z = lax.rem(data, 2), lax.rem(data // 2, 4), data // 8
    started = []
    loads = []

    def peer(dx, dz, dy, dc):
        chip = lax.rem(z + dz + 4, 4) * 4 + lax.rem(y + dy + 4, 4)
        return lax.rem(x + dx, 4), chip * 2 + lax.rem(core + dc, 2)

    def ring_a(step, other=0):
        role = core if not other else 1 - core
        return peer(0, step * role, step * (1 - role), other)

    def ring_b(step):
        return peer(0, step * (1 - core), step * core, 0)

    def column(da, db, other=0):
        role = core if not other else 1 - core
        dy, dz = da * (1 - role) + db * role, da * role + db * (1 - role)
        slab = (lax.rem(z + dz + 4, 4) * 4 + lax.rem(y + dy + 4, 4)) * 2 + role
        return pl.multiple_of(slab * SLAB, SLAB)

    def slab_of(ref, da, db, other=0):
        return ref.at[:, :, pl.ds(column(da, db, other), SLAB)]

    def half_of(ref, da, db, half):
        return ref.at[:, :, pl.ds(pl.multiple_of(column(da, db) + half * HALF, HALF), HALF)]

    def remote(src, dst, device):
        index = len(started)
        copy = pltpu.make_async_remote_copy(src_ref=src, dst_ref=dst, send_sem=send_sem.at[index], recv_sem=recv_sem.at[index], device_id=device, device_id_type=MESH)
        copy.start()
        started.append(copy)
        return copy

    def load(src, dst):
        copy = pltpu.make_async_copy(src, dst, load_sem.at[len(loads)])
        copy.start()
        loads.append(copy)
        return copy

    def columns_loop(body, init=0, start=0, length=SLAB):
        def step(index, carry):
            return body(pl.ds(pl.multiple_of(start + index * STEP_COLS, 128), STEP_COLS), carry)
        return lax.fori_loop(0, length // STEP_COLS, step, init)

    def add_into(target, terms, start=0, length=SLAB, shift=0):
        def body(cols, carry):
            for tile in range(TILES):
                total = None
                for term in terms:
                    value = term[tile, :, cols].astype(jnp.float32)
                    total = value if total is None else total + value
                target[tile, :, cols] = total
            return carry
        columns_loop(body, 0, start, length)

    peers = [(0, 0, k, 0) for k in (1, 2, 3)] + [(0, k, 0, 0) for k in (1, 2, 3)]
    peers += [(0, 0, k, 1) for k in (1, 3)] + [(0, k, 0, 1) for k in (1, 3)]
    peers += [group for sum_round in SUM_ROUNDS for group in sum_round if group not in peers]
    if (0, 0, 0, 1) not in peers:
        peers.append((0, 0, 0, 1))
    barrier = pltpu.get_barrier_semaphore()
    for offsets in peers:
        pl.semaphore_signal(barrier, inc=1, device_id=peer(*offsets), device_id_type=MESH)

    order = [(1, db) for db in MINUS_SET] + [(3, db) for db in PLUS_SET] + [(1, PLUS_SET[0]), (3, MINUS_SET[0]), (1, PLUS_SET[1]), (3, MINUS_SET[1])]
    order += [(0, db) for db in (2, 3, 0, 1)]
    place = {key: index for index, key in enumerate(order)}
    own_load = {key: load(slab_of(grads, *key), own_raw.at[place[key]]) for key in order}
    state_load = [load(src, dst) for src, dst in ((master_in, master), (one_in, one), (two_in, two))]

    pl.semaphore_wait(barrier, len(peers))

    raw_copy = {}
    for index in range(2):
        for sign, group in ((1, PLUS_SET), (-1, MINUS_SET)):
            for other in (0, 1):
                buffer = relay_raw.at[0 if sign == 1 else 1, other, index]
                raw_copy[sign, other, index] = remote(slab_of(grads, 2, group[index], other), buffer, ring_a(sign, other))
    pair_copy = {key: remote(slab_of(grads, *key, other=1), pair_raw.at[place[key]], peer(0, 0, 0, 1)) for key in order}

    for copy in state_load:
        copy.wait()

    def weight_square(cols, carry):
        return tuple(carry[tile] + master[tile, :, cols] * master[tile, :, cols] for tile in range(TILES))

    def fold(value):
        parts = [value[:, 128 * k:128 * (k + 1)] for k in range(STEP_COLS // 128)]
        while len(parts) > 1:
            parts = [left + right for left, right in zip(parts[::2], parts[1::2])] + parts[len(parts) - len(parts) % 2:]
        return parts[0]

    zero = jnp.zeros((8, STEP_COLS), jnp.float32)
    weight_sq = [jnp.sum(fold(value), axis=1, keepdims=True) for value in columns_loop(weight_square, (zero,) * TILES)]

    def pair_terms(key):
        own_load[key].wait()
        pair_copy[key].wait_recv()
        return [own_raw.at[place[key]], pair_raw.at[place[key]]]

    fin_copy = {}
    for index in range(2):
        for sign, da, group in ((1, 1, MINUS_SET), (-1, 3, PLUS_SET)):
            db, side = group[index], 0 if sign == 1 else 1
            add_into(early.at[side, index], pair_terms((da, db)))
            fin_copy[sign, db] = remote(early.at[side, index], fin.at[side, db], ring_a(sign))
    for index in range(2):
        for sign, da, group in ((1, 1, PLUS_SET), (-1, 3, MINUS_SET)):
            db, side = group[index], 0 if sign == 1 else 1
            terms = pair_terms((da, db))
            for other in (0, 1):
                raw_copy[sign, other, index].wait_recv()
                terms.append(relay_raw.at[side, other, index])
            add_into(late.at[side, index], terms)
            fin_copy[sign, db] = remote(late.at[side, index], fin.at[side, db], ring_a(sign))

    def first_sum(db):
        terms = pair_terms((0, db))
        for sign in (1, -1):
            fin_copy[sign, db].wait_recv()
            terms.append(fin.at[0 if sign == 1 else 1, db])
        add_into(sums.at[db], terms)

    def half(ref, index):
        return ref.at[:, :, pl.ds(index * HALF, HALF)]

    first_sum(2)
    mid_plus = remote(half(sums.at[2], 0), mid.at[0], ring_b(1))
    mid_minus = remote(half(sums.at[2], 1), mid.at[1], ring_b(-1))
    first_sum(3)
    end_minus = [remote(half(sums.at[3], 0), half(end.at[1], 0), ring_b(-1))]
    first_sum(1)
    end_plus = [remote(half(sums.at[1], 1), half(end.at[0], 1), ring_b(1))]

    def add_half(target, extra, half_index):
        def body(index, carry):
            cols = pl.ds(pl.multiple_of(index * STEP_COLS, 128), STEP_COLS)
            wide = pl.ds(pl.multiple_of(half_index * HALF + index * STEP_COLS, 128), STEP_COLS)
            for tile in range(TILES):
                target[tile, :, wide] = target[tile, :, wide] + extra[tile, :, cols]
            return carry
        lax.fori_loop(0, HALF // STEP_COLS, body, 0)

    mid_plus.wait_recv()
    add_half(sums.at[1], mid.at[0], 0)
    end_plus.append(remote(half(sums.at[1], 0), half(end.at[0], 0), ring_b(1)))
    mid_minus.wait_recv()
    add_half(sums.at[3], mid.at[1], 1)
    end_minus.append(remote(half(sums.at[3], 1), half(end.at[1], 1), ring_b(-1)))
    first_sum(0)
    for copy in end_plus + end_minus:
        copy.wait_recv()

    def gather_sum(cols, carry):
        for tile in range(TILES):
            total = sums[0, tile, :, cols] + end[0, tile, :, cols] + end[1, tile, :, cols]
            grad_sum[tile, :, cols] = total
            carry = carry + total * total
        return carry

    def global_sum(first, value):
        for index, group in enumerate(SUM_ROUNDS):
            tiles[first + index] = value
            copies = [remote(tiles.at[first + index], slots.at[first + index, slot], peer(*offsets)) for slot, offsets in enumerate(group)]
            for copy in copies:
                copy.wait_recv()
            for slot in range(len(group)):
                value = value + slots[first + index, slot]
        return value

    grad_sq = global_sum(0, fold(columns_loop(gather_sum, zero)))
    norm_sq = jnp.sum(jnp.sum(grad_sq, axis=0, keepdims=True), axis=1, keepdims=True) / (REPLICAS * REPLICAS)
    clip = jnp.minimum(1.0, MAX_NORM / jnp.sqrt(norm_sq)) / REPLICAS

    def moments(cols, carry):
        squares = []
        for tile in range(TILES):
            scaled = clip * grad_sum[tile, :, cols]
            new_one = BETA_ONE * one[tile, :, cols] + (1.0 - BETA_ONE) * scaled
            new_two = BETA_TWO * two[tile, :, cols] + (1.0 - BETA_TWO) * scaled * scaled
            step = (new_one / CORR_ONE) / (jnp.sqrt(new_two / CORR_TWO) + EPSILON) + WEIGHT_DECAY * master[tile, :, cols]
            one_out[tile, :, cols] = new_one
            two_out[tile, :, cols] = new_two
            direction[tile, :, cols] = step
            squares.append(carry[tile] + step * step)
        return tuple(squares)

    step_sq = [jnp.sum(fold(value), axis=1, keepdims=True) for value in columns_loop(moments, (zero,) * TILES)]

    lane = lax.broadcasted_iota(jnp.int32, (8, 128), 1)
    sub = lax.broadcasted_iota(jnp.int32, (8, 128), 0)
    row_sums = jnp.zeros((8, 128), jnp.float32)
    for index, value in enumerate(step_sq + weight_sq):
        row_sums = jnp.where(lane == index, value, row_sums)

    def tensor_of(sublane):
        row = 8 * jnp.where(lane >= 3, lane - 3, lane) + sublane
        layer = jnp.where(row >= 12, 1, 0)
        block = row - 12 * layer
        return 4 * layer + jnp.where(block >= 3, 1, 0) + jnp.where(block >= 4, 1, 0) + jnp.where(block >= 8, 1, 0)

    row_sums = global_sum(len(SUM_ROUNDS), row_sums)
    tensor_sums = row_sums
    for shift in range(1, 8):
        moved = jnp.where(sub >= shift, sub - shift, sub - shift + 8)
        tensor_sums = tensor_sums + jnp.where(tensor_of(moved) == tensor_of(sub), pltpu.roll(row_sums, shift, 0), 0.0)
    norms = jnp.sqrt(tensor_sums)
    ratio = pltpu.roll(norms, 125, 1) / norms
    rate = [LEARN_RATE * jnp.sum(jnp.where(lane == tile, ratio, 0.0), axis=1, keepdims=True) for tile in range(TILES)]

    own_column = column(0, 0)

    def weights(index, carry):
        cols = pl.ds(pl.multiple_of(index * STEP_COLS, 128), STEP_COLS)
        wide = pl.ds(pl.multiple_of(own_column + index * STEP_COLS, 128), STEP_COLS)
        for tile in range(TILES):
            value = master[tile, :, cols] - rate[tile] * direction[tile, :, cols]
            master_out[tile, :, cols] = value
            params[tile, :, wide] = value.astype(jnp.bfloat16)
        return carry

    lax.fori_loop(0, SLAB // STEP_COLS, weights, 0)

    handed = []

    def spread(ref):
        return remote(ref, ref, ring_a(1)), remote(ref, ref, ring_a(-1))

    def hand(ref):
        handed.append(remote(ref, ref, peer(0, 0, 0, 1)))

    mine = slab_of(params, 0, 0)
    ring_copy = remote(mine, mine, ring_b(1)), remote(mine, mine, ring_b(-1))
    spread_copy = {0: spread(mine)}
    hand(mine)
    far = []
    for side, db in ((0, 3), (1, 1)):
        ring_copy[side].wait_recv()
        far.append(remote(half_of(params, 0, db, side), half_of(params, 0, db, side), ring_b(1 if side == 0 else -1)))
        spread_copy[db] = spread(slab_of(params, 0, db))
        hand(slab_of(params, 0, db))

    def relay(db):
        for side, da in ((0, 3), (1, 1)):
            spread_copy[db][side].wait_recv()
            ref = half_of(params, da, db, side)
            relayed.append((da, db, side, remote(ref, ref, ring_a(1 if side == 0 else -1))))
            hand(slab_of(params, da, db))

    relayed = []
    relay(0)
    far_spread = []
    for side in (0, 1):
        far[side].wait_recv()
        far_spread.append(spread(half_of(params, 0, 2, side)))
        hand(half_of(params, 0, 2, side))
    relay(3)
    relay(1)
    for half_index in (0, 1):
        for side, da in ((0, 3), (1, 1)):
            far_spread[half_index][side].wait_recv()
            ref = half_of(params, da, 2, half_index)
            if side == half_index:
                relayed.append((da, 2, side, remote(ref, ref, ring_a(1 if side == 0 else -1))))
            hand(ref)
    for da, db, side, copy in relayed:
        copy.wait_recv()
        hand(half_of(params, 2, db, side))
    for copy in handed:
        copy.wait_recv()
    for copy in started:
        copy.wait_send()


def solution(mesh):
    state_spec = P(None, ('model', 'data'))

    def device_step(local_grads, master, moment_one, moment_two):
        state = (TILES, 8, SLAB)
        width = local_grads.shape[2]
        hbm = pl.BlockSpec(memory_space=pltpu.HBM)
        vmem = pl.BlockSpec(memory_space=pltpu.VMEM)

        def slabs(count, dtype, length=SLAB):
            return pltpu.VMEM(count + (TILES, 8, length), dtype)

        outs = pl.pallas_call(
            lamb_kernel,
            name='lamb_step',
            out_shape=(
                jax.ShapeDtypeStruct((TILES, 8, width), jnp.bfloat16),
                jax.ShapeDtypeStruct(state, jnp.float32),
                jax.ShapeDtypeStruct(state, jnp.float32),
                jax.ShapeDtypeStruct(state, jnp.float32),
            ),
            in_specs=[hbm] * 4,
            out_specs=(vmem,) * 4,
            scratch_shapes=[
                slabs((12,), jnp.bfloat16),
                slabs((12,), jnp.bfloat16),
                slabs((2, 2, 2), jnp.bfloat16),
                slabs((2, 2), jnp.float32),
                slabs((2, 2), jnp.float32),
                slabs((2, 4), jnp.float32),
                slabs((4,), jnp.float32),
                slabs((2,), jnp.float32, HALF),
                slabs((2,), jnp.float32),
                slabs((), jnp.float32),
                slabs((), jnp.float32),
                slabs((), jnp.float32),
                slabs((), jnp.float32),
                slabs((), jnp.float32),
                pltpu.VMEM((2 * len(SUM_ROUNDS), 8, 128), jnp.float32),
                pltpu.VMEM((2 * len(SUM_ROUNDS), SLOTS, 8, 128), jnp.float32),
                pltpu.SemaphoreType.DMA((COPIES,)),
                pltpu.SemaphoreType.DMA((COPIES,)),
                pltpu.SemaphoreType.DMA((LOADS,)),
            ],
            compiler_params=pltpu.CompilerParams(collective_id=0, has_side_effects=True),
        )(
            local_grads.reshape(TILES, 8, width),
            master.reshape(state),
            moment_one.reshape(state),
            moment_two.reshape(state),
        )
        return tuple(out.reshape(24, -1) for out in outs)

    return jax.shard_map(device_step, mesh=mesh, in_specs=(P('data', None, 'model'), state_spec, state_spec, state_spec), out_specs=(P(None, 'model'), state_spec, state_spec, state_spec), check_vma=False)
```

```python
import functools

import jax
import jax.numpy as jnp
from jax import lax
from jax.experimental import pallas as pl
from jax.experimental.pallas import tpu as pltpu
from jax.sharding import PartitionSpec as P

STEP = 4
LEARN_RATE = 0.08
BETA_ONE = 0.9
BETA_TWO = 0.999
EPSILON = 1e-6
WEIGHT_DECAY = 0.01
MAX_NORM = 1.0
CORR_ONE = 1.0 - BETA_ONE ** STEP
CORR_TWO = 1.0 - BETA_TWO ** STEP

MESH = pl.DeviceIdType.MESH
TILES = 3
SLAB = 4608
HALF = SLAB // 2
STEP_COLS = 768
REPLICAS = 32
PLUS_SET = (2, 0)
MINUS_SET = (3, 1)
SUM_ROUNDS = (
    tuple((0, 0, k, 0) for k in (1, 2, 3)),
    tuple((0, k, 0, 0) for k in (1, 2, 3)),
    tuple((k, 0, 0, e) for k in (0, 1, 2, 3) for e in (0, 1) if (k, e) != (0, 0)),
)
SLOTS = max(len(group) for group in SUM_ROUNDS)
COPIES = 120
LOADS = 18
VMEM_LIMIT = 40 * 2 ** 20


def lamb_kernel(grads, master_in, one_in, two_in, params, master_out, one_out, two_out, own_raw, pair_raw, relay_raw, early, late, fin, sums, mid, end, master, one, two, grad_sum, direction, tiles, slots, send_sem, recv_sem, load_sem):
    x, data = lax.axis_index('model'), lax.axis_index('data')
    core, y, z = lax.rem(data, 2), lax.rem(data // 2, 4), data // 8
    started = []
    loads = []

    def peer(dx, dz, dy, dc):
        chip = lax.rem(z + dz + 4, 4) * 4 + lax.rem(y + dy + 4, 4)
        return lax.rem(x + dx, 4), chip * 2 + lax.rem(core + dc, 2)

    def ring_a(step, other=0):
        role = core if not other else 1 - core
        return peer(0, step * role, step * (1 - role), other)

    def ring_b(step):
        return peer(0, step * (1 - core), step * core, 0)

    def column(da, db, other=0):
        role = core if not other else 1 - core
        dy, dz = da * (1 - role) + db * role, da * role + db * (1 - role)
        slab = (lax.rem(z + dz + 4, 4) * 4 + lax.rem(y + dy + 4, 4)) * 2 + role
        return pl.multiple_of(slab * SLAB, SLAB)

    def slab_of(ref, da, db, other=0):
        return ref.at[:, :, pl.ds(column(da, db, other), SLAB)]

    def half_of(ref, da, db, half):
        return ref.at[:, :, pl.ds(pl.multiple_of(column(da, db) + half * HALF, HALF), HALF)]

    def remote(src, dst, device):
        index = len(started)
        copy = pltpu.make_async_remote_copy(src_ref=src, dst_ref=dst, send_sem=send_sem.at[index], recv_sem=recv_sem.at[index], device_id=device, device_id_type=MESH)
        copy.start()
        started.append(copy)
        return copy

    def load(src, dst):
        copy = pltpu.make_async_copy(src, dst, load_sem.at[len(loads)])
        copy.start()
        loads.append(copy)
        return copy

    def columns_loop(body, init=0, start=0, length=SLAB):
        def step(index, carry):
            return body(pl.ds(pl.multiple_of(start + index * STEP_COLS, 128), STEP_COLS), carry)
        return lax.fori_loop(0, length // STEP_COLS, step, init)

    def add_into(target, terms, start=0, length=SLAB, shift=0):
        def body(cols, carry):
            for tile in range(TILES):
                total = None
                for term in terms:
                    value = term[tile, :, cols].astype(jnp.float32)
                    total = value if total is None else total + value
                target[tile, :, cols] = total
            return carry
        columns_loop(body, 0, start, length)

    peers = [(0, 0, k, 0) for k in (1, 2, 3)] + [(0, k, 0, 0) for k in (1, 2, 3)]
    peers += [(0, 0, k, 1) for k in (1, 3)] + [(0, k, 0, 1) for k in (1, 3)]
    peers += [group for sum_round in SUM_ROUNDS for group in sum_round if group not in peers]
    if (0, 0, 0, 1) not in peers:
        peers.append((0, 0, 0, 1))
    barrier = pltpu.get_barrier_semaphore()
    for offsets in peers:
        pl.semaphore_signal(barrier, inc=1, device_id=peer(*offsets), device_id_type=MESH)

    order = [(1, db) for db in MINUS_SET] + [(3, db) for db in PLUS_SET] + [(1, PLUS_SET[0]), (3, MINUS_SET[0]), (1, PLUS_SET[1]), (3, MINUS_SET[1])]
    order += [(0, db) for db in (2, 3, 0, 1)]
    place = {key: index for index, key in enumerate(order)}
    own_load = {key: load(slab_of(grads, *key), own_raw.at[place[key]]) for key in order}
    state_load = [load(src, dst) for src, dst in ((master_in, master), (one_in, one), (two_in, two))]

    pl.semaphore_wait(barrier, len(peers))

    raw_copy = {}
    for index in range(2):
        for sign, group in ((1, PLUS_SET), (-1, MINUS_SET)):
            for other in (0, 1):
                buffer = relay_raw.at[0 if sign == 1 else 1, other, index]
                raw_copy[sign, other, index] = remote(slab_of(grads, 2, group[index], other), buffer, ring_a(sign, other))
    pair_copy = {key: remote(slab_of(grads, *key, other=1), pair_raw.at[place[key]], peer(0, 0, 0, 1)) for key in order}

    for copy in state_load:
        copy.wait()

    def weight_square(cols, carry):
        return tuple(carry[tile] + master[tile, :, cols] * master[tile, :, cols] for tile in range(TILES))

    def fold(value):
        parts = [value[:, 128 * k:128 * (k + 1)] for k in range(STEP_COLS // 128)]
        while len(parts) > 1:
            parts = [left + right for left, right in zip(parts[::2], parts[1::2])] + parts[len(parts) - len(parts) % 2:]
        return parts[0]

    zero = jnp.zeros((8, STEP_COLS), jnp.float32)
    weight_sq = [jnp.sum(fold(value), axis=1, keepdims=True) for value in columns_loop(weight_square, (zero,) * TILES)]

    def pair_terms(key):
        own_load[key].wait()
        pair_copy[key].wait_recv()
        return [own_raw.at[place[key]], pair_raw.at[place[key]]]

    fin_copy = {}
    for index in range(2):
        for sign, da, group in ((1, 1, MINUS_SET), (-1, 3, PLUS_SET)):
            db, side = group[index], 0 if sign == 1 else 1
            add_into(early.at[side, index], pair_terms((da, db)))
            fin_copy[sign, db] = remote(early.at[side, index], fin.at[side, db], ring_a(sign))
    for index in range(2):
        for sign, da, group in ((1, 1, PLUS_SET), (-1, 3, MINUS_SET)):
            db, side = group[index], 0 if sign == 1 else 1
            terms = pair_terms((da, db))
            for other in (0, 1):
                raw_copy[sign, other, index].wait_recv()
                terms.append(relay_raw.at[side, other, index])
            add_into(late.at[side, index], terms)
            fin_copy[sign, db] = remote(late.at[side, index], fin.at[side, db], ring_a(sign))

    def first_sum(db):
        terms = pair_terms((0, db))
        for sign in (1, -1):
            fin_copy[sign, db].wait_recv()
            terms.append(fin.at[0 if sign == 1 else 1, db])
        add_into(sums.at[db], terms)

    def half(ref, index):
        return ref.at[:, :, pl.ds(index * HALF, HALF)]

    first_sum(2)
    mid_plus = remote(half(sums.at[2], 0), mid.at[0], ring_b(1))
    mid_minus = remote(half(sums.at[2], 1), mid.at[1], ring_b(-1))
    first_sum(3)
    end_minus = [remote(half(sums.at[3], 0), half(end.at[1], 0), ring_b(-1))]
    first_sum(1)
    end_plus = [remote(half(sums.at[1], 1), half(end.at[0], 1), ring_b(1))]

    def add_half(target, extra, half_index):
        def body(index, carry):
            cols = pl.ds(pl.multiple_of(index * STEP_COLS, 128), STEP_COLS)
            wide = pl.ds(pl.multiple_of(half_index * HALF + index * STEP_COLS, 128), STEP_COLS)
            for tile in range(TILES):
                target[tile, :, wide] = target[tile, :, wide] + extra[tile, :, cols]
            return carry
        lax.fori_loop(0, HALF // STEP_COLS, body, 0)

    mid_plus.wait_recv()
    add_half(sums.at[1], mid.at[0], 0)
    end_plus.append(remote(half(sums.at[1], 0), half(end.at[0], 0), ring_b(1)))
    mid_minus.wait_recv()
    add_half(sums.at[3], mid.at[1], 1)
    end_minus.append(remote(half(sums.at[3], 1), half(end.at[1], 1), ring_b(-1)))
    first_sum(0)
    for copy in end_plus + end_minus:
        copy.wait_recv()

    def gather_sum(cols, carry):
        for tile in range(TILES):
            total = sums[0, tile, :, cols] + end[0, tile, :, cols] + end[1, tile, :, cols]
            grad_sum[tile, :, cols] = total
            carry = carry + total * total
        return carry

    def global_sum(first, value):
        for index, group in enumerate(SUM_ROUNDS):
            tiles[first + index] = value
            copies = [remote(tiles.at[first + index], slots.at[first + index, slot], peer(*offsets)) for slot, offsets in enumerate(group)]
            for copy in copies:
                copy.wait_recv()
            for slot in range(len(group)):
                value = value + slots[first + index, slot]
        return value

    grad_sq = global_sum(0, fold(columns_loop(gather_sum, zero)))
    norm_sq = jnp.sum(jnp.sum(grad_sq, axis=0, keepdims=True), axis=1, keepdims=True) / (REPLICAS * REPLICAS)
    clip = jnp.minimum(1.0, MAX_NORM / jnp.sqrt(norm_sq)) / REPLICAS

    def moments(cols, carry):
        squares = []
        for tile in range(TILES):
            scaled = clip * grad_sum[tile, :, cols]
            new_one = BETA_ONE * one[tile, :, cols] + (1.0 - BETA_ONE) * scaled
            new_two = BETA_TWO * two[tile, :, cols] + (1.0 - BETA_TWO) * scaled * scaled
            step = (new_one / CORR_ONE) / (jnp.sqrt(new_two / CORR_TWO) + EPSILON) + WEIGHT_DECAY * master[tile, :, cols]
            one_out[tile, :, cols] = new_one
            two_out[tile, :, cols] = new_two
            direction[tile, :, cols] = step
            squares.append(carry[tile] + step * step)
        return tuple(squares)

    step_sq = [jnp.sum(fold(value), axis=1, keepdims=True) for value in columns_loop(moments, (zero,) * TILES)]

    lane = lax.broadcasted_iota(jnp.int32, (8, 128), 1)
    sub = lax.broadcasted_iota(jnp.int32, (8, 128), 0)
    row_sums = jnp.zeros((8, 128), jnp.float32)
    for index, value in enumerate(step_sq + weight_sq):
        row_sums = jnp.where(lane == index, value, row_sums)

    def tensor_of(sublane):
        row = 8 * jnp.where(lane >= 3, lane - 3, lane) + sublane
        layer = jnp.where(row >= 12, 1, 0)
        block = row - 12 * layer
        return 4 * layer + jnp.where(block >= 3, 1, 0) + jnp.where(block >= 4, 1, 0) + jnp.where(block >= 8, 1, 0)

    row_sums = global_sum(len(SUM_ROUNDS), row_sums)
    tensor_sums = row_sums
    for shift in range(1, 8):
        moved = jnp.where(sub >= shift, sub - shift, sub - shift + 8)
        tensor_sums = tensor_sums + jnp.where(tensor_of(moved) == tensor_of(sub), pltpu.roll(row_sums, shift, 0), 0.0)
    norms = jnp.sqrt(tensor_sums)
    ratio = pltpu.roll(norms, 125, 1) / norms
    rate = [LEARN_RATE * jnp.sum(jnp.where(lane == tile, ratio, 0.0), axis=1, keepdims=True) for tile in range(TILES)]

    own_column = column(0, 0)

    def weights(index, carry):
        cols = pl.ds(pl.multiple_of(index * STEP_COLS, 128), STEP_COLS)
        wide = pl.ds(pl.multiple_of(own_column + index * STEP_COLS, 128), STEP_COLS)
        for tile in range(TILES):
            value = master[tile, :, cols] - rate[tile] * direction[tile, :, cols]
            master_out[tile, :, cols] = value
            params[tile, :, wide] = value.astype(jnp.bfloat16)
        return carry

    lax.fori_loop(0, SLAB // STEP_COLS, weights, 0)

    handed = []

    def spread(ref):
        return remote(ref, ref, ring_a(1)), remote(ref, ref, ring_a(-1))

    def hand(ref):
        handed.append(remote(ref, ref, peer(0, 0, 0, 1)))

    mine = slab_of(params, 0, 0)
    ring_copy = remote(mine, mine, ring_b(1)), remote(mine, mine, ring_b(-1))
    spread_copy = {0: spread(mine)}
    hand(mine)
    far = []
    for side, db in ((0, 3), (1, 1)):
        ring_copy[side].wait_recv()
        far.append(remote(half_of(params, 0, db, side), half_of(params, 0, db, side), ring_b(1 if side == 0 else -1)))
        spread_copy[db] = spread(slab_of(params, 0, db))
        hand(slab_of(params, 0, db))

    def relay(db):
        for side, da in ((0, 3), (1, 1)):
            spread_copy[db][side].wait_recv()
            ref = half_of(params, da, db, side)
            relayed.append((da, db, side, remote(ref, ref, ring_a(1 if side == 0 else -1))))
            hand(slab_of(params, da, db))

    relayed = []
    relay(0)
    far_spread = []
    for side in (0, 1):
        far[side].wait_recv()
        far_spread.append(spread(half_of(params, 0, 2, side)))
        hand(half_of(params, 0, 2, side))
    relay(3)
    relay(1)
    for half_index in (0, 1):
        for side, da in ((0, 3), (1, 1)):
            far_spread[half_index][side].wait_recv()
            ref = half_of(params, da, 2, half_index)
            if side == half_index:
                relayed.append((da, 2, side, remote(ref, ref, ring_a(1 if side == 0 else -1))))
            hand(ref)
    for da, db, side, copy in relayed:
        copy.wait_recv()
        hand(half_of(params, 2, db, side))
    for copy in handed:
        copy.wait_recv()
    for copy in started:
        copy.wait_send()


def solution(mesh):
    state_spec = P(None, ('model', 'data'))

    def device_step(local_grads, master, moment_one, moment_two):
        state = (TILES, 8, SLAB)
        width = local_grads.shape[2]
        hbm = pl.BlockSpec(memory_space=pltpu.HBM)
        vmem = pl.BlockSpec(memory_space=pltpu.VMEM)

        def slabs(count, dtype, length=SLAB):
            return pltpu.VMEM(count + (TILES, 8, length), dtype)

        operands = (local_grads.reshape(TILES, 8, width), master.reshape(state), moment_one.reshape(state), moment_two.reshape(state))
        outs = pl.pallas_call(
            lamb_kernel,
            name='lamb_step',
            out_shape=(
                pltpu.VMEM((TILES, 8, width), jnp.bfloat16),
                pltpu.VMEM(state, jnp.float32),
                pltpu.VMEM(state, jnp.float32),
                pltpu.VMEM(state, jnp.float32),
            ),
            in_specs=[hbm] * 4,
            out_specs=(vmem,) * 4,
            scratch_shapes=[
                slabs((12,), jnp.bfloat16),
                slabs((12,), jnp.bfloat16),
                slabs((2, 2, 2), jnp.bfloat16),
                slabs((2, 2), jnp.float32),
                slabs((2, 2), jnp.float32),
                slabs((2, 4), jnp.float32),
                slabs((4,), jnp.float32),
                slabs((2,), jnp.float32, HALF),
                slabs((2,), jnp.float32),
                slabs((), jnp.float32),
                slabs((), jnp.float32),
                slabs((), jnp.float32),
                slabs((), jnp.float32),
                slabs((), jnp.float32),
                pltpu.VMEM((2 * len(SUM_ROUNDS), 8, 128), jnp.float32),
                pltpu.VMEM((2 * len(SUM_ROUNDS), SLOTS, 8, 128), jnp.float32),
                pltpu.SemaphoreType.DMA((COPIES,)),
                pltpu.SemaphoreType.DMA((COPIES,)),
                pltpu.SemaphoreType.DMA((LOADS,)),
            ],
            compiler_params=pltpu.CompilerParams(collective_id=0, has_side_effects=True, vmem_limit_bytes=VMEM_LIMIT),
        )(
            *(pltpu.with_memory_space_constraint(operand, pltpu.HBM) for operand in operands)
        )
        return tuple(out.reshape(24, -1) for out in outs)

    return jax.shard_map(device_step, mesh=mesh, in_specs=(P('data', None, 'model'), state_spec, state_spec, state_spec), out_specs=(P(None, 'model'), state_spec, state_spec, state_spec), check_vma=False)
```

```python
import functools

import jax
import jax.numpy as jnp
from jax import lax
from jax.experimental import pallas as pl
from jax.experimental.pallas import tpu as pltpu
from jax.sharding import PartitionSpec as P

STEP = 4
LEARN_RATE = 0.08
BETA_ONE = 0.9
BETA_TWO = 0.999
EPSILON = 1e-6
WEIGHT_DECAY = 0.01
MAX_NORM = 1.0
CORR_ONE = 1.0 - BETA_ONE ** STEP
CORR_TWO = 1.0 - BETA_TWO ** STEP

MESH = pl.DeviceIdType.MESH
TILES = 3
SLAB = 4608
HALF = SLAB // 2
STEP_COLS = 768
REPLICAS = 32
LATE = (((2, 0), (1, 1), (1, 0), (0, 0)), ((2, 1), (3, 0), (3, 1), (0, 1)))
EARLY = (((3, 0), (3, 1), (2, 1), (0, 1)), ((1, 1), (1, 0), (2, 0), (0, 0)))
PIECES = 4
ORDER = ((1, 3), (3, 1), (1, 2), (3, 2), (1, 0), (3, 0), (1, 1), (3, 3), (0, 2), (0, 1), (0, 3), (0, 0))
PLANE = tuple((0, k, e, 0) for k in range(4) for e in range(4) if (k, e) != (0, 0))
ACROSS = tuple((k, 0, 0, e) for k in range(4) for e in range(2) if (k, e) != (0, 0))
SUM_ROUNDS = (PLANE, ACROSS)
SLOTS = len(PLANE)
BARRIER = ACROSS + tuple((0, k, 0, e) for k in (1, 3) for e in (0, 1)) + tuple((0, 0, k, e) for k in (1, 3) for e in (0, 1))
COPIES = 180
LOADS = len(ORDER) + 3
VMEM_LIMIT = 40 * 2 ** 20
WRITE_PIECES = 4


def lamb_kernel(grads, master_in, one_in, two_in, params, master_out, one_out, two_out, own_raw, pair_raw, relay_raw, early, late, fin, sums, mid, end, master, one, two, grad_sum, direction, rows, slots, send_sem, recv_sem, load_sem):
    x, data = lax.axis_index('model'), lax.axis_index('data')
    core, y, z = lax.rem(data, 2), lax.rem(data // 2, 4), data // 8
    started = []
    loads = []

    def peer(dx, dz, dy, dc):
        chip = lax.rem(z + dz + 4, 4) * 4 + lax.rem(y + dy + 4, 4)
        return lax.rem(x + dx, 4), chip * 2 + lax.rem(core + dc, 2)

    def ring_a(side, other=0):
        role = core if not other else 1 - core
        step = 1 - 2 * side
        return peer(0, step * role, step * (1 - role), other)

    def ring_b(side):
        step = 1 - 2 * side
        return peer(0, step * (1 - core), step * core, 0)

    partner = peer(0, 0, 0, 1)

    def column(da, db, other=0):
        role = core if not other else 1 - core
        dy, dz = da * (1 - role) + db * role, da * role + db * (1 - role)
        slab = (lax.rem(z + dz, 4) * 4 + lax.rem(y + dy, 4)) * 2 + role
        return pl.multiple_of(slab * SLAB, SLAB)

    def whole(ref, da, db, other=0):
        return ref.at[:, :, pl.ds(column(da, db, other), SLAB)]

    def piece(ref, da, db, half, other=0):
        return ref.at[:, :, pl.ds(pl.multiple_of(column(da, db, other) + half * HALF, HALF), HALF)]

    def part(ref, half):
        return ref.at[:, :, pl.ds(half * HALF, HALF)]

    def remote(src, dst, device):
        index = len(started)
        copy = pltpu.make_async_remote_copy(src_ref=src, dst_ref=dst, send_sem=send_sem.at[index], recv_sem=recv_sem.at[index], device_id=device, device_id_type=MESH)
        copy.start()
        started.append(copy)
        return copy

    def load(src, dst):
        copy = pltpu.make_async_copy(src, dst, load_sem.at[len(loads)])
        copy.start()
        loads.append(copy)
        return copy

    def columns_loop(body, init=0, length=SLAB):
        def step(index, carry):
            return body(index * STEP_COLS, carry)
        return lax.fori_loop(0, length // STEP_COLS, step, init)

    def at(start):
        return pl.ds(pl.multiple_of(start, 128), STEP_COLS)

    def add_half(target, target_start, terms):
        def body(offset, carry):
            for tile in range(TILES):
                total = None
                for term, start in terms:
                    value = term[tile, :, at(start + offset)].astype(jnp.float32)
                    total = value if total is None else total + value
                target[tile, :, at(target_start + offset)] = total
            return carry
        columns_loop(body, 0, HALF)

    barrier = pltpu.get_barrier_semaphore()
    for offsets in BARRIER:
        pl.semaphore_signal(barrier, inc=1, device_id=peer(*offsets), device_id_type=MESH)

    place = {key: index for index, key in enumerate(ORDER)}
    own_load = {key: load(whole(grads, *key), own_raw.at[place[key]]) for key in ORDER}
    state_load = [load(src, dst) for src, dst in ((master_in, master), (one_in, one), (two_in, two))]

    pl.semaphore_wait(barrier, len(BARRIER))

    raw_copy = {}
    for index in range(PIECES):
        for side in (0, 1):
            for other in (0, 1):
                db, half = LATE[side][index]
                raw_copy[side, other, index] = remote(piece(grads, 2, db, half, other), relay_raw.at[side, other, index], ring_a(side, other))
    pair_copy = {key: remote(whole(grads, *key, other=1), pair_raw.at[place[key]], partner) for key in ORDER}

    def fold(value):
        parts = [value[:, 128 * k:128 * (k + 1)] for k in range(STEP_COLS // 128)]
        while len(parts) > 1:
            parts = [left + right for left, right in zip(parts[::2], parts[1::2])] + parts[len(parts) - len(parts) % 2:]
        return parts[0]

    def weight_square(offset, carry):
        return tuple(carry[tile] + master[tile, :, at(offset)] * master[tile, :, at(offset)] for tile in range(TILES))

    for copy in state_load:
        copy.wait()
    zero = jnp.zeros((8, STEP_COLS), jnp.float32)
    weight_sq = [jnp.sum(fold(value), axis=1, keepdims=True) for value in columns_loop(weight_square, (zero,) * TILES)]

    ready = set()

    def pair_terms(da, db, half):
        key = (da, db)
        if key not in ready:
            own_load[key].wait()
            pair_copy[key].wait_recv()
            ready.add(key)
        return [(own_raw.at[place[key]], half * HALF), (pair_raw.at[place[key]], half * HALF)]

    fin_copy = {}
    for index in range(PIECES):
        for side in (0, 1):
            db, half = EARLY[side][index]
            add_half(early.at[side, index], 0, pair_terms(1 + 2 * side, db, half))
            fin_copy[side, db, half] = remote(early.at[side, index], part(fin.at[side, db], half), ring_a(side))
    for index in range(PIECES):
        for side in (0, 1):
            db, half = LATE[side][index]
            terms = pair_terms(1 + 2 * side, db, half)
            for other in (0, 1):
                raw_copy[side, other, index].wait_recv()
                terms.append((relay_raw.at[side, other, index], 0))
            add_half(late.at[side, index], 0, terms)
            fin_copy[side, db, half] = remote(late.at[side, index], part(fin.at[side, db], half), ring_a(side))

    def first_sum(db, half):
        terms = pair_terms(0, db, half)
        for side in (0, 1):
            fin_copy[side, db, half].wait_recv()
            terms.append((fin.at[side, db], half * HALF))
        add_half(sums.at[db], half * HALF, terms)

    mid_copy = {}
    end_copy = {}
    for side in (0, 1):
        first_sum(2, side)
        mid_copy[side] = remote(part(sums.at[2], side), mid.at[side], ring_b(side))
    for side in (0, 1):
        db, half = 1 + 2 * side, 1 - side
        first_sum(db, half)
        end_copy[side, half] = remote(part(sums.at[db], half), part(end.at[side], half), ring_b(side))
    for side in (0, 1):
        first_sum(1 + 2 * side, side)
    for side in (0, 1):
        db = 1 + 2 * side
        mid_copy[side].wait_recv()
        add_half(sums.at[db], side * HALF, [(sums.at[db], side * HALF), (mid.at[side], 0)])
        end_copy[side, side] = remote(part(sums.at[db], side), part(end.at[side], side), ring_b(side))
    for side in (0, 1):
        first_sum(0, side)
    for side in (0, 1):
        end_copy[side, 1 - side].wait_recv()
    for side in (0, 1):
        end_copy[side, side].wait_recv()

    def gather_sum(offset, carry):
        for tile in range(TILES):
            total = sums[0, tile, :, at(offset)] + end[0, tile, :, at(offset)] + end[1, tile, :, at(offset)]
            grad_sum[tile, :, at(offset)] = total
            carry = carry + total * total
        return carry

    def global_sum(first, value):
        for index, group in enumerate(SUM_ROUNDS):
            rows[first + index] = value
            copies = [remote(rows.at[first + index], slots.at[first + index, slot], peer(*offsets)) for slot, offsets in enumerate(group)]
            for copy in copies:
                copy.wait_recv()
            received = [slots[first + index, slot] for slot in range(len(group))] + [value]
            while len(received) > 1:
                received = [left + right for left, right in zip(received[::2], received[1::2])]
            value = received[0]
        return value

    grad_sq = global_sum(0, jnp.sum(fold(columns_loop(gather_sum, zero)), axis=0, keepdims=True))
    norm_sq = jnp.sum(grad_sq, axis=1, keepdims=True) / (REPLICAS * REPLICAS)
    clip = jnp.minimum(1.0, MAX_NORM / jnp.sqrt(norm_sq)) / REPLICAS

    def moments(offset, carry):
        squares = []
        for tile in range(TILES):
            scaled = clip * grad_sum[tile, :, at(offset)]
            new_one = BETA_ONE * one[tile, :, at(offset)] + (1.0 - BETA_ONE) * scaled
            new_two = BETA_TWO * two[tile, :, at(offset)] + (1.0 - BETA_TWO) * scaled * scaled
            step = (new_one * (1.0 / CORR_ONE)) / (jnp.sqrt(new_two * (1.0 / CORR_TWO)) + EPSILON) + WEIGHT_DECAY * master[tile, :, at(offset)]
            one_out[tile, :, at(offset)] = new_one
            two_out[tile, :, at(offset)] = new_two
            direction[tile, :, at(offset)] = step
            squares.append(carry[tile] + step * step)
        return tuple(squares)

    step_sq = [jnp.sum(fold(value), axis=1, keepdims=True) for value in columns_loop(moments, (zero,) * TILES)]

    lane = lax.broadcasted_iota(jnp.int32, (8, 128), 1)
    sub = lax.broadcasted_iota(jnp.int32, (8, 128), 0)
    spread_sums = jnp.zeros((8, 128), jnp.float32)
    for tile in range(TILES):
        spread_sums = jnp.where(lane == 8 * tile + sub, step_sq[tile], spread_sums)
        spread_sums = jnp.where(lane == 32 + 8 * tile + sub, weight_sq[tile], spread_sums)

    def tensor_of(row):
        layer = jnp.where(row >= 12, 1, 0)
        block = row - 12 * layer
        return 4 * layer + jnp.where(block >= 3, 1, 0) + jnp.where(block >= 4, 1, 0) + jnp.where(block >= 8, 1, 0)

    row_sums = jnp.broadcast_to(global_sum(len(SUM_ROUNDS), jnp.sum(spread_sums, axis=0, keepdims=True)), (8, 128))
    rate = []
    for tile in range(TILES):
        tensor = tensor_of(8 * tile + sub)
        step_mask = (tensor_of(lane) == tensor) & (lane < 24)
        weight_mask = (tensor_of(lane - 32) == tensor) & (lane >= 32) & (lane < 56)
        step_norm = jnp.sqrt(jnp.sum(jnp.where(step_mask, row_sums, 0.0), axis=1, keepdims=True))
        weight_norm = jnp.sqrt(jnp.sum(jnp.where(weight_mask, row_sums, 0.0), axis=1, keepdims=True))
        rate.append(LEARN_RATE * (weight_norm / step_norm))

    own_column = column(0, 0)

    def weights(offset, carry):
        for tile in range(TILES):
            value = master[tile, :, at(offset)] - rate[tile] * direction[tile, :, at(offset)]
            master_out[tile, :, at(offset)] = value
            params[tile, :, at(own_column + offset)] = value.astype(jnp.bfloat16)
        return carry

    columns_loop(weights)

    handed = []
    along_b = {}
    along_a = {}
    far_b = {}
    far_a = {}

    def send(da, db, half, device):
        ref = piece(params, da, db, half)
        return remote(ref, ref, device)

    def hand(da, db, half):
        handed.append(send(da, db, half, partner))

    def pass_on(first, second):
        for one_piece, other_piece in ((first, second), (second, first)):
            along_a[0, one_piece] = send(0, *one_piece, ring_a(0))
            along_a[1, other_piece] = send(0, *other_piece, ring_a(1))

    for order in (0, 1):
        for side in (0, 1):
            half = side if order == 0 else 1 - side
            along_b[side, half] = send(0, 0, half, ring_b(side))
        for side in (0, 1):
            half = side if order == 0 else 1 - side
            along_a[side, (0, half)] = send(0, 0, half, ring_a(side))
    hand(0, 0, 0)
    hand(0, 0, 1)

    def arrived(side, db, half):
        along_a[side, (db, half)].wait_recv()
        da = 3 - 2 * side
        if half == side:
            far_a[db, half] = send(da, db, half, ring_a(side))
        hand(da, db, half)

    for side in (0, 1):
        db = 3 - 2 * side
        along_b[side, side].wait_recv()
        far_b[side] = send(0, db, side, ring_b(side))
    pass_on((3, 0), (1, 1))
    hand(0, 3, 0)
    hand(0, 1, 1)
    for side in (0, 1):
        arrived(side, 0, side)
    for side in (0, 1):
        along_b[side, 1 - side].wait_recv()
    pass_on((1, 0), (3, 1))
    hand(0, 3, 1)
    hand(0, 1, 0)
    for side in (0, 1):
        arrived(side, 0, 1 - side)
    for side in (0, 1):
        far_b[side].wait_recv()
    pass_on((2, 0), (2, 1))
    hand(0, 2, 0)
    hand(0, 2, 1)
    for pieces in (((3, 0), (1, 1)), ((1, 1), (3, 0)), ((1, 0), (3, 1)), ((3, 1), (1, 0)), ((2, 0), (2, 1)), ((2, 1), (2, 0))):
        for side in (0, 1):
            arrived(side, *pieces[side])
    for db in (0, 3, 1, 2):
        for half in (0, 1):
            far_a[db, half].wait_recv()
            hand(2, db, half)
    for copy in handed:
        copy.wait_recv()
    for copy in started:
        copy.wait_send()


def write_kernel(params, master, one, two, params_out, master_out, one_out, two_out, sem):
    pairs = [(master, master_out), (one, one_out), (two, two_out)]
    width = params.shape[2] // WRITE_PIECES
    for tile in range(TILES):
        for index in range(WRITE_PIECES):
            cols = pl.ds(index * width, width)
            pairs.append((params.at[tile, :, cols], params_out.at[tile, :, cols]))
    copies = [pltpu.make_async_copy(src, dst, sem.at[index]) for index, (src, dst) in enumerate(pairs)]
    for copy in copies:
        copy.start()
    for copy in copies:
        copy.wait()


def solution(mesh):
    state_spec = P(None, ('model', 'data'))

    def device_step(local_grads, master, moment_one, moment_two):
        state = (TILES, 8, SLAB)
        width = local_grads.shape[2]
        hbm = pl.BlockSpec(memory_space=pltpu.HBM)
        vmem = pl.BlockSpec(memory_space=pltpu.VMEM)

        def slabs(count, dtype, length=SLAB):
            return pltpu.VMEM(count + (TILES, 8, length), dtype)

        operands = (local_grads.reshape(TILES, 8, width), master.reshape(state), moment_one.reshape(state), moment_two.reshape(state))
        results = pl.pallas_call(
            lamb_kernel,
            name='lamb_step',
            out_shape=(
                pltpu.VMEM((TILES, 8, width), jnp.bfloat16),
                pltpu.VMEM(state, jnp.float32),
                pltpu.VMEM(state, jnp.float32),
                pltpu.VMEM(state, jnp.float32),
            ),
            in_specs=[hbm] * 4,
            out_specs=(vmem,) * 4,
            scratch_shapes=[
                slabs((len(ORDER),), jnp.bfloat16),
                slabs((len(ORDER),), jnp.bfloat16),
                slabs((2, 2, PIECES), jnp.bfloat16, HALF),
                slabs((2, PIECES), jnp.float32, HALF),
                slabs((2, PIECES), jnp.float32, HALF),
                slabs((2, 4), jnp.float32),
                slabs((4,), jnp.float32),
                slabs((2,), jnp.float32, HALF),
                slabs((2,), jnp.float32),
                slabs((), jnp.float32),
                slabs((), jnp.float32),
                slabs((), jnp.float32),
                slabs((), jnp.float32),
                slabs((), jnp.float32),
                pltpu.VMEM((2 * len(SUM_ROUNDS), 1, 128), jnp.float32),
                pltpu.VMEM((2 * len(SUM_ROUNDS), SLOTS, 1, 128), jnp.float32),
                pltpu.SemaphoreType.DMA((COPIES,)),
                pltpu.SemaphoreType.DMA((COPIES,)),
                pltpu.SemaphoreType.DMA((LOADS,)),
            ],
            compiler_params=pltpu.CompilerParams(collective_id=0, has_side_effects=True, vmem_limit_bytes=VMEM_LIMIT),
        )(*(pltpu.with_memory_space_constraint(operand, pltpu.HBM) for operand in operands))
        outs = pl.pallas_call(
            write_kernel,
            name='write_out',
            out_shape=tuple(pltpu.HBM(result.shape, result.dtype) for result in results),
            in_specs=[vmem] * 4,
            out_specs=(hbm,) * 4,
            scratch_shapes=[pltpu.SemaphoreType.DMA((TILES * WRITE_PIECES + 3,))],
            compiler_params=pltpu.CompilerParams(vmem_limit_bytes=2 ** 20),
        )(*results)
        return tuple(out.reshape(24, -1) for out in outs)

    return jax.shard_map(device_step, mesh=mesh, in_specs=(P('data', None, 'model'), state_spec, state_spec, state_spec), out_specs=(P(None, 'model'), state_spec, state_spec, state_spec), check_vma=False)
```

```python
import functools

import jax
import jax.numpy as jnp
from jax import lax
from jax.experimental import pallas as pl
from jax.experimental.pallas import tpu as pltpu
from jax.sharding import PartitionSpec as P

STEP = 4
LEARN_RATE = 0.08
BETA_ONE = 0.9
BETA_TWO = 0.999
EPSILON = 1e-6
WEIGHT_DECAY = 0.01
MAX_NORM = 1.0
CORR_ONE = 1.0 - BETA_ONE ** STEP
CORR_TWO = 1.0 - BETA_TWO ** STEP

MESH = pl.DeviceIdType.MESH
TILES = 3
SLAB = 4608
HALF = SLAB // 2
STEP_COLS = 768
REPLICAS = 32
LATE = (((2, 0), (1, 1), (1, 0), (0, 0)), ((2, 1), (3, 0), (3, 1), (0, 1)))
EARLY = (((3, 0), (3, 1), (2, 1), (0, 1)), ((1, 1), (1, 0), (2, 0), (0, 0)))
PIECES = 4
ORDER = ((1, 3), (3, 1), (1, 2), (3, 2), (1, 0), (3, 0), (1, 1), (3, 3), (0, 2), (0, 1), (0, 3), (0, 0))
EVERY = sorted(((i, j, k, e) for i in range(4) for j in range(4) for k in range(4) for e in range(2) if i + j + k + e), key=lambda far: -sum(min(step, 4 - step) for step in far[:3]) - far[3] / 2)
DEVICES = len(EVERY) + 1
ALONG_X = tuple((k, 0, 0, 0) for k in (1, 3))
ALONG_Z = tuple((0, k, 0, 0) for k in (1, 3))
ALONG_Y = tuple((0, 0, k, 0) for k in (1, 3))
OTHER_CORE = ((0, 0, 0, 1),)
BARRIER = ALONG_X + ALONG_Z + ALONG_Y + OTHER_CORE + tuple((0, k, 0, 1) for k in (1, 3)) + tuple((0, 0, k, 1) for k in (1, 3))
STAGES = (ALONG_X, OTHER_CORE, ALONG_Y, ALONG_Y, ALONG_Z, ALONG_Z)
COPIES = 120
LOADS = len(ORDER) + 3
VMEM_LIMIT = 40 * 2 ** 20
WRITE_PIECES = 4


def lamb_kernel(grads, master_in, one_in, two_in, params, master_out, one_out, two_out, own_raw, pair_raw, relay_raw, early, late, fin, sums, mid, end, master, one, two, grad_sum, direction, rows, slots, send_sem, recv_sem, load_sem, sum_send, sum_recv, stage_sem):
    x, data = lax.axis_index('model'), lax.axis_index('data')
    core, y, z = lax.rem(data, 2), lax.rem(data // 2, 4), data // 8
    started = []
    loads = []

    def peer(dx, dz, dy, dc):
        chip = lax.rem(z + dz + 4, 4) * 4 + lax.rem(y + dy + 4, 4)
        return lax.rem(x + dx, 4), chip * 2 + lax.rem(core + dc, 2)

    def ring_a(side, other=0):
        role = core if not other else 1 - core
        step = 1 - 2 * side
        return peer(0, step * role, step * (1 - role), other)

    def ring_b(side):
        step = 1 - 2 * side
        return peer(0, step * (1 - core), step * core, 0)

    partner = peer(0, 0, 0, 1)

    def column(da, db, other=0):
        role = core if not other else 1 - core
        dy, dz = da * (1 - role) + db * role, da * role + db * (1 - role)
        slab = (lax.rem(z + dz, 4) * 4 + lax.rem(y + dy, 4)) * 2 + role
        return pl.multiple_of(slab * SLAB, SLAB)

    def whole(ref, da, db, other=0):
        return ref.at[:, :, pl.ds(column(da, db, other), SLAB)]

    def piece(ref, da, db, half, other=0):
        return ref.at[:, :, pl.ds(pl.multiple_of(column(da, db, other) + half * HALF, HALF), HALF)]

    def part(ref, half):
        return ref.at[:, :, pl.ds(half * HALF, HALF)]

    def remote(src, dst, device):
        index = len(started)
        copy = pltpu.make_async_remote_copy(src_ref=src, dst_ref=dst, send_sem=send_sem.at[index], recv_sem=recv_sem.at[index], device_id=device, device_id_type=MESH)
        copy.start()
        started.append(copy)
        return copy

    def load(src, dst):
        copy = pltpu.make_async_copy(src, dst, load_sem.at[len(loads)])
        copy.start()
        loads.append(copy)
        return copy

    def columns_loop(body, init=0, length=SLAB):
        def step(index, carry):
            return body(index * STEP_COLS, carry)
        return lax.fori_loop(0, length // STEP_COLS, step, init)

    def at(start):
        return pl.ds(pl.multiple_of(start, 128), STEP_COLS)

    def add_half(target, target_start, terms):
        def body(offset, carry):
            for tile in range(TILES):
                total = None
                for term, start in terms:
                    value = term[tile, :, at(start + offset)].astype(jnp.float32)
                    total = value if total is None else total + value
                target[tile, :, at(target_start + offset)] = total
            return carry
        columns_loop(body, 0, HALF)

    barrier = pltpu.get_barrier_semaphore()
    for offsets in BARRIER:
        pl.semaphore_signal(barrier, inc=1, device_id=peer(*offsets), device_id_type=MESH)

    def stage_signal(stage):
        for offsets in STAGES[stage]:
            pl.semaphore_signal(stage_sem.at[stage], inc=1, device_id=peer(*offsets), device_id_type=MESH)

    def stage_next(stage):
        pl.semaphore_wait(stage_sem.at[stage], len(STAGES[stage]))
        if stage + 1 < len(STAGES):
            stage_signal(stage + 1)

    place = {key: index for index, key in enumerate(ORDER)}
    own_load = {key: load(whole(grads, *key), own_raw.at[place[key]]) for key in ORDER}
    state_load = [load(src, dst) for src, dst in ((master_in, master), (one_in, one), (two_in, two))]

    pl.semaphore_wait(barrier, len(BARRIER))

    raw_copy = {}
    for index in range(PIECES):
        for side in (0, 1):
            for other in (0, 1):
                db, half = LATE[side][index]
                raw_copy[side, other, index] = remote(piece(grads, 2, db, half, other), relay_raw.at[side, other, index], ring_a(side, other))
    pair_copy = {key: remote(whole(grads, *key, other=1), pair_raw.at[place[key]], partner) for key in ORDER}

    stage_signal(0)

    def fold(value):
        parts = [value[:, 128 * k:128 * (k + 1)] for k in range(STEP_COLS // 128)]
        while len(parts) > 1:
            parts = [left + right for left, right in zip(parts[::2], parts[1::2])] + parts[len(parts) - len(parts) % 2:]
        return parts[0]

    def weight_square(offset, carry):
        return tuple(carry[tile] + master[tile, :, at(offset)] * master[tile, :, at(offset)] for tile in range(TILES))

    for copy in state_load:
        copy.wait()
    zero = jnp.zeros((8, STEP_COLS), jnp.float32)
    weight_sq = [jnp.sum(fold(value), axis=1, keepdims=True) for value in columns_loop(weight_square, (zero,) * TILES)]

    ready = set()

    def pair_terms(da, db, half):
        key = (da, db)
        if key not in ready:
            own_load[key].wait()
            pair_copy[key].wait_recv()
            ready.add(key)
        return [(own_raw.at[place[key]], half * HALF), (pair_raw.at[place[key]], half * HALF)]

    fin_copy = {}
    for index in range(PIECES):
        for side in (0, 1):
            db, half = EARLY[side][index]
            add_half(early.at[side, index], 0, pair_terms(1 + 2 * side, db, half))
            fin_copy[side, db, half] = remote(early.at[side, index], part(fin.at[side, db], half), ring_a(side))
        stage_next(index)
    for index in range(PIECES):
        for side in (0, 1):
            db, half = LATE[side][index]
            terms = pair_terms(1 + 2 * side, db, half)
            for other in (0, 1):
                raw_copy[side, other, index].wait_recv()
                terms.append((relay_raw.at[side, other, index], 0))
            add_half(late.at[side, index], 0, terms)
            fin_copy[side, db, half] = remote(late.at[side, index], part(fin.at[side, db], half), ring_a(side))
        if PIECES + index < len(STAGES):
            stage_next(PIECES + index)

    def first_sum(db, half):
        terms = pair_terms(0, db, half)
        for side in (0, 1):
            fin_copy[side, db, half].wait_recv()
            terms.append((fin.at[side, db], half * HALF))
        add_half(sums.at[db], half * HALF, terms)

    mid_copy = {}
    end_copy = {}
    for side in (0, 1):
        first_sum(2, side)
        mid_copy[side] = remote(part(sums.at[2], side), mid.at[side], ring_b(side))
    for side in (0, 1):
        db, half = 1 + 2 * side, 1 - side
        first_sum(db, half)
        end_copy[side, half] = remote(part(sums.at[db], half), part(end.at[side], half), ring_b(side))
    for side in (0, 1):
        first_sum(1 + 2 * side, side)
    for side in (0, 1):
        db = 1 + 2 * side
        mid_copy[side].wait_recv()
        add_half(sums.at[db], side * HALF, [(sums.at[db], side * HALF), (mid.at[side], 0)])
        end_copy[side, side] = remote(part(sums.at[db], side), part(end.at[side], side), ring_b(side))
    for side in (0, 1):
        first_sum(0, side)
    for side in (0, 1):
        end_copy[side, 1 - side].wait_recv()
    for side in (0, 1):
        end_copy[side, side].wait_recv()

    def gather_sum(offset, carry):
        for tile in range(TILES):
            total = sums[0, tile, :, at(offset)] + end[0, tile, :, at(offset)] + end[1, tile, :, at(offset)]
            grad_sum[tile, :, at(offset)] = total
            carry = carry + total * total
        return carry

    mine_index = (x * 4 + z) * 8 + y * 2 + core
    sum_sent = []

    def global_sum(which, value):
        rows[which] = value
        slots[which, mine_index] = value
        for offsets in EVERY:
            pltpu.make_async_remote_copy(src_ref=rows.at[which], dst_ref=slots.at[which, mine_index], send_sem=sum_send.at[which], recv_sem=sum_recv.at[which], device_id=peer(*offsets), device_id_type=MESH).start()
        block = slots.at[which, pl.ds(0, len(EVERY))]
        total = pltpu.make_async_remote_copy(src_ref=block, dst_ref=block, send_sem=sum_send.at[which], recv_sem=sum_recv.at[which], device_id=partner, device_id_type=MESH)
        total.wait_recv()
        sum_sent.append(total)
        received = [slots[which, slot] for slot in range(DEVICES)]
        while len(received) > 1:
            received = [left + right for left, right in zip(received[::2], received[1::2])]
        return received[0]

    grad_sq = global_sum(0, jnp.sum(fold(columns_loop(gather_sum, zero)), axis=0, keepdims=True))
    norm_sq = jnp.sum(grad_sq, axis=1, keepdims=True) / (REPLICAS * REPLICAS)
    clip = jnp.minimum(1.0, MAX_NORM / jnp.sqrt(norm_sq)) / REPLICAS

    def moments(offset, carry):
        squares = []
        for tile in range(TILES):
            scaled = clip * grad_sum[tile, :, at(offset)]
            new_one = BETA_ONE * one[tile, :, at(offset)] + (1.0 - BETA_ONE) * scaled
            new_two = BETA_TWO * two[tile, :, at(offset)] + (1.0 - BETA_TWO) * scaled * scaled
            step = (new_one * (1.0 / CORR_ONE)) / (jnp.sqrt(new_two * (1.0 / CORR_TWO)) + EPSILON) + WEIGHT_DECAY * master[tile, :, at(offset)]
            one_out[tile, :, at(offset)] = new_one
            two_out[tile, :, at(offset)] = new_two
            direction[tile, :, at(offset)] = step
            squares.append(carry[tile] + step * step)
        return tuple(squares)

    step_sq = [jnp.sum(fold(value), axis=1, keepdims=True) for value in columns_loop(moments, (zero,) * TILES)]

    lane = lax.broadcasted_iota(jnp.int32, (8, 128), 1)
    sub = lax.broadcasted_iota(jnp.int32, (8, 128), 0)
    spread_sums = jnp.zeros((8, 128), jnp.float32)
    for tile in range(TILES):
        spread_sums = jnp.where(lane == 8 * tile + sub, step_sq[tile], spread_sums)
        spread_sums = jnp.where(lane == 32 + 8 * tile + sub, weight_sq[tile], spread_sums)

    def tensor_of(row):
        layer = jnp.where(row >= 12, 1, 0)
        block = row - 12 * layer
        return 4 * layer + jnp.where(block >= 3, 1, 0) + jnp.where(block >= 4, 1, 0) + jnp.where(block >= 8, 1, 0)

    row_sums = jnp.broadcast_to(global_sum(1, jnp.sum(spread_sums, axis=0, keepdims=True)), (8, 128))
    rate = []
    for tile in range(TILES):
        tensor = tensor_of(8 * tile + sub)
        step_mask = (tensor_of(lane) == tensor) & (lane < 24)
        weight_mask = (tensor_of(lane - 32) == tensor) & (lane >= 32) & (lane < 56)
        step_norm = jnp.sqrt(jnp.sum(jnp.where(step_mask, row_sums, 0.0), axis=1, keepdims=True))
        weight_norm = jnp.sqrt(jnp.sum(jnp.where(weight_mask, row_sums, 0.0), axis=1, keepdims=True))
        rate.append(LEARN_RATE * (weight_norm / step_norm))

    own_column = column(0, 0)

    def weights(offset, carry):
        for tile in range(TILES):
            value = master[tile, :, at(offset)] - rate[tile] * direction[tile, :, at(offset)]
            master_out[tile, :, at(offset)] = value
            params[tile, :, at(own_column + offset)] = value.astype(jnp.bfloat16)
        return carry

    columns_loop(weights)

    handed = []
    along_b = {}
    along_a = {}
    far_b = {}
    far_a = {}

    def send(da, db, half, device):
        ref = piece(params, da, db, half)
        return remote(ref, ref, device)

    def hand(da, db, half):
        handed.append(send(da, db, half, partner))

    def pass_on(first, second):
        for one_piece, other_piece in ((first, second), (second, first)):
            along_a[0, one_piece] = send(0, *one_piece, ring_a(0))
            along_a[1, other_piece] = send(0, *other_piece, ring_a(1))

    for order in (0, 1):
        for side in (0, 1):
            half = side if order == 0 else 1 - side
            along_b[side, half] = send(0, 0, half, ring_b(side))
        for side in (0, 1):
            half = side if order == 0 else 1 - side
            along_a[side, (0, half)] = send(0, 0, half, ring_a(side))
    hand(0, 0, 0)
    hand(0, 0, 1)

    def arrived(side, db, half):
        along_a[side, (db, half)].wait_recv()
        da = 3 - 2 * side
        if half == side:
            far_a[db, half] = send(da, db, half, ring_a(side))
        hand(da, db, half)

    for side in (0, 1):
        db = 3 - 2 * side
        along_b[side, side].wait_recv()
        far_b[side] = send(0, db, side, ring_b(side))
    pass_on((3, 0), (1, 1))
    hand(0, 3, 0)
    hand(0, 1, 1)
    for side in (0, 1):
        arrived(side, 0, side)
    for side in (0, 1):
        along_b[side, 1 - side].wait_recv()
    pass_on((1, 0), (3, 1))
    hand(0, 3, 1)
    hand(0, 1, 0)
    for side in (0, 1):
        arrived(side, 0, 1 - side)
    for side in (0, 1):
        far_b[side].wait_recv()
    pass_on((2, 0), (2, 1))
    hand(0, 2, 0)
    hand(0, 2, 1)
    for pieces in (((3, 0), (1, 1)), ((1, 1), (3, 0)), ((1, 0), (3, 1)), ((3, 1), (1, 0)), ((2, 0), (2, 1)), ((2, 1), (2, 0))):
        for side in (0, 1):
            arrived(side, *pieces[side])
    for db in (0, 3, 1, 2):
        for half in (0, 1):
            far_a[db, half].wait_recv()
            hand(2, db, half)
    for copy in handed:
        copy.wait_recv()
    for copy in started + sum_sent:
        copy.wait_send()


def write_kernel(params, master, one, two, params_out, master_out, one_out, two_out, sem):
    pairs = [(master, master_out), (one, one_out), (two, two_out)]
    width = params.shape[2] // WRITE_PIECES
    for tile in range(TILES):
        for index in range(WRITE_PIECES):
            cols = pl.ds(index * width, width)
            pairs.append((params.at[tile, :, cols], params_out.at[tile, :, cols]))
    copies = [pltpu.make_async_copy(src, dst, sem.at[index]) for index, (src, dst) in enumerate(pairs)]
    for copy in copies:
        copy.start()
    for copy in copies:
        copy.wait()


def solution(mesh):
    state_spec = P(None, ('model', 'data'))

    def device_step(local_grads, master, moment_one, moment_two):
        state = (TILES, 8, SLAB)
        width = local_grads.shape[2]
        hbm = pl.BlockSpec(memory_space=pltpu.HBM)
        vmem = pl.BlockSpec(memory_space=pltpu.VMEM)

        def slabs(count, dtype, length=SLAB):
            return pltpu.VMEM(count + (TILES, 8, length), dtype)

        operands = (local_grads.reshape(TILES, 8, width), master.reshape(state), moment_one.reshape(state), moment_two.reshape(state))
        results = pl.pallas_call(
            lamb_kernel,
            name='lamb_step',
            out_shape=(
                pltpu.VMEM((TILES, 8, width), jnp.bfloat16),
                pltpu.VMEM(state, jnp.float32),
                pltpu.VMEM(state, jnp.float32),
                pltpu.VMEM(state, jnp.float32),
            ),
            in_specs=[hbm] * 4,
            out_specs=(vmem,) * 4,
            scratch_shapes=[
                slabs((len(ORDER),), jnp.bfloat16),
                slabs((len(ORDER),), jnp.bfloat16),
                slabs((2, 2, PIECES), jnp.bfloat16, HALF),
                slabs((2, PIECES), jnp.float32, HALF),
                slabs((2, PIECES), jnp.float32, HALF),
                slabs((2, 4), jnp.float32),
                slabs((4,), jnp.float32),
                slabs((2,), jnp.float32, HALF),
                slabs((2,), jnp.float32),
                slabs((), jnp.float32),
                slabs((), jnp.float32),
                slabs((), jnp.float32),
                slabs((), jnp.float32),
                slabs((), jnp.float32),
                pltpu.VMEM((2, 1, 128), jnp.float32),
                pltpu.VMEM((2, DEVICES, 1, 128), jnp.float32),
                pltpu.SemaphoreType.DMA((COPIES,)),
                pltpu.SemaphoreType.DMA((COPIES,)),
                pltpu.SemaphoreType.DMA((LOADS,)),
                pltpu.SemaphoreType.DMA((2,)),
                pltpu.SemaphoreType.DMA((2,)),
                pltpu.SemaphoreType.REGULAR((len(STAGES),)),
            ],
            compiler_params=pltpu.CompilerParams(collective_id=0, has_side_effects=True, vmem_limit_bytes=VMEM_LIMIT),
        )(*(pltpu.with_memory_space_constraint(operand, pltpu.HBM) for operand in operands))
        outs = pl.pallas_call(
            write_kernel,
            name='write_out',
            out_shape=tuple(pltpu.HBM(result.shape, result.dtype) for result in results),
            in_specs=[vmem] * 4,
            out_specs=(hbm,) * 4,
            scratch_shapes=[pltpu.SemaphoreType.DMA((TILES * WRITE_PIECES + 3,))],
            compiler_params=pltpu.CompilerParams(vmem_limit_bytes=2 ** 20),
        )(*results)
        return tuple(out.reshape(24, -1) for out in outs)

    return jax.shard_map(device_step, mesh=mesh, in_specs=(P('data', None, 'model'), state_spec, state_spec, state_spec), out_specs=(P(None, 'model'), state_spec, state_spec, state_spec), check_vma=False)
```

```python
import functools

import jax
import jax.numpy as jnp
from jax import lax
from jax.experimental import pallas as pl
from jax.experimental.pallas import tpu as pltpu
from jax.sharding import PartitionSpec as P

STEP = 4
LEARN_RATE = 0.08
BETA_ONE = 0.9
BETA_TWO = 0.999
EPSILON = 1e-6
WEIGHT_DECAY = 0.01
MAX_NORM = 1.0
CORR_ONE = 1.0 - BETA_ONE ** STEP
CORR_TWO = 1.0 - BETA_TWO ** STEP

MESH = pl.DeviceIdType.MESH
TILES = 3
SLAB = 4608
HALF = SLAB // 2
QUARTER = SLAB // 4
STEP_COLS = 768
REPLICAS = 32
LATE = (((2, 0), (1, 1), (1, 0), (0, 0)), ((2, 1), (3, 0), (3, 1), (0, 1)))
EARLY = (((3, 0), (3, 1), (2, 1), (0, 1)), ((1, 1), (1, 0), (2, 0), (0, 0)))
PIECES = 4
ORDER = ((1, 3), (3, 1), (1, 2), (3, 2), (1, 0), (3, 0), (1, 1), (3, 3), (0, 2), (0, 1), (0, 3), (0, 0))
EVERY = sorted(((i, j, k, e) for i in range(4) for j in range(4) for k in range(4) for e in range(2) if i + j + k + e), key=lambda far: -sum(min(step, 4 - step) for step in far[:3]) - far[3] / 2)
DEVICES = len(EVERY) + 1
ALONG_X = tuple((k, 0, 0, 0) for k in (1, 3))
ALONG_Z = tuple((0, k, 0, 0) for k in (1, 3))
ALONG_Y = tuple((0, 0, k, 0) for k in (1, 3))
OTHER_CORE = ((0, 0, 0, 1),)
BARRIER = ALONG_X + ALONG_Z + ALONG_Y + OTHER_CORE + tuple((0, k, 0, 1) for k in (1, 3)) + tuple((0, 0, k, 1) for k in (1, 3))
STAGES = (ALONG_X, OTHER_CORE, ALONG_Y, ALONG_Y, ALONG_Z, ALONG_Z)
GROUPS = ('raw', 'pair', 'early', 'late', 'mid', 'end', 'weight', 'step', 'gather')
AHEAD = ('weight', 'step')
COPIES = 82
LOADS = len(ORDER) + 3
VMEM_LIMIT = 40 * 2 ** 20
WRITE_PIECES = 4


def lamb_kernel(grads, master_in, one_in, two_in, params, master_out, one_out, two_out, own_raw, pair_raw, relay_raw, early, late, fin, sums, mid, end, master, one, two, grad_sum, direction, ahead_weight, ahead_step, rows, slots, send_sem, recv_sem, load_sem, sum_send, sum_recv, hand_sems, stage_sem):
    x, data = lax.axis_index('model'), lax.axis_index('data')
    core, y, z = lax.rem(data, 2), lax.rem(data // 2, 4), data // 8
    started = []
    gathered = []
    loads = []

    def peer(dx, dz, dy, dc):
        chip = lax.rem(z + dz + 4, 4) * 4 + lax.rem(y + dy + 4, 4)
        return lax.rem(x + dx, 4), chip * 2 + lax.rem(core + dc, 2)

    def ring_a(side, other=0):
        role = core if not other else 1 - core
        step = 1 - 2 * side
        return peer(0, step * role, step * (1 - role), other)

    def ring_b(side):
        step = 1 - 2 * side
        return peer(0, step * (1 - core), step * core, 0)

    partner = peer(0, 0, 0, 1)

    def column(da, db, other=0):
        role = core if not other else 1 - core
        dy, dz = da * (1 - role) + db * role, da * role + db * (1 - role)
        slab = (lax.rem(z + dz, 4) * 4 + lax.rem(y + dy, 4)) * 2 + role
        return pl.multiple_of(slab * SLAB, SLAB)

    def whole(ref, da, db, other=0):
        return ref.at[:, :, pl.ds(column(da, db, other), SLAB)]

    def piece(ref, da, db, half, other=0):
        return ref.at[:, :, pl.ds(pl.multiple_of(column(da, db, other) + half * HALF, HALF), HALF)]

    def part(ref, half):
        return ref.at[:, :, pl.ds(half * HALF, HALF)]

    def remote(src, dst, device, group='gather', landing=None):
        if landing is None:
            landing = recv_sem.at[len(started)]
            started.append(group)
        if group == 'gather':
            gathered.append(src.shape[-1])
        copy = pltpu.make_async_remote_copy(src_ref=src, dst_ref=dst, send_sem=send_sem.at[GROUPS.index(group)], recv_sem=landing, device_id=device, device_id_type=MESH)
        copy.start()
        return copy

    def all_of(ref, group='gather', landing=None):
        landing = recv_sem.at[0] if landing is None else landing
        return pltpu.make_async_remote_copy(src_ref=ref, dst_ref=ref, send_sem=send_sem.at[GROUPS.index(group)], recv_sem=landing, device_id=partner, device_id_type=MESH)

    def load(src, dst):
        copy = pltpu.make_async_copy(src, dst, load_sem.at[len(loads)])
        copy.start()
        loads.append(copy)
        return copy

    def columns_loop(body, init=0, length=SLAB):
        def step(index, carry):
            return body(index * STEP_COLS, carry)
        return lax.fori_loop(0, length // STEP_COLS, step, init)

    def at(start):
        return pl.ds(pl.multiple_of(start, 128), STEP_COLS)

    def add_half(target, target_start, terms):
        def body(offset, carry):
            for tile in range(TILES):
                total = None
                for term, start in terms:
                    value = term[tile, :, at(start + offset)].astype(jnp.float32)
                    total = value if total is None else total + value
                target[tile, :, at(target_start + offset)] = total
            return carry
        columns_loop(body, 0, HALF)

    barrier = pltpu.get_barrier_semaphore()
    for offsets in BARRIER:
        pl.semaphore_signal(barrier, inc=1, device_id=peer(*offsets), device_id_type=MESH)

    def stage_signal(stage):
        for offsets in STAGES[stage]:
            pl.semaphore_signal(stage_sem.at[stage], inc=1, device_id=peer(*offsets), device_id_type=MESH)

    def stage_next(stage):
        pl.semaphore_wait(stage_sem.at[stage], len(STAGES[stage]))
        if stage + 1 < len(STAGES):
            stage_signal(stage + 1)

    place = {key: index for index, key in enumerate(ORDER)}
    own_load = {key: load(whole(grads, *key), own_raw.at[place[key]]) for key in ORDER}
    state_load = [load(src, dst) for src, dst in ((master_in, master), (one_in, one), (two_in, two))]

    pl.semaphore_wait(barrier, len(BARRIER))

    raw_copy = {}
    for index in range(PIECES):
        for side in (0, 1):
            for other in (0, 1):
                db, half = LATE[side][index]
                raw_copy[side, other, index] = remote(piece(grads, 2, db, half, other), relay_raw.at[side, other, index], ring_a(side, other), 'raw')
    pair_copy = {key: remote(whole(grads, *key, other=1), pair_raw.at[place[key]], partner, 'pair') for key in ORDER}

    stage_signal(0)

    def fold(value):
        parts = [value[:, 128 * k:128 * (k + 1)] for k in range(STEP_COLS // 128)]
        while len(parts) > 1:
            parts = [left + right for left, right in zip(parts[::2], parts[1::2])] + parts[len(parts) - len(parts) % 2:]
        return parts[0]

    def weight_square(offset, carry):
        return tuple(carry[tile] + master[tile, :, at(offset)] * master[tile, :, at(offset)] for tile in range(TILES))

    for copy in state_load:
        copy.wait()
    zero = jnp.zeros((8, STEP_COLS), jnp.float32)
    weight_sq = [jnp.sum(fold(value), axis=1, keepdims=True) for value in columns_loop(weight_square, (zero,) * TILES)]

    ready = set()

    def pair_terms(da, db, half):
        key = (da, db)
        if key not in ready:
            own_load[key].wait()
            pair_copy[key].wait_recv()
            ready.add(key)
        return [(own_raw.at[place[key]], half * HALF), (pair_raw.at[place[key]], half * HALF)]

    fin_copy = {}
    for index in range(PIECES):
        for side in (0, 1):
            db, half = EARLY[side][index]
            add_half(early.at[side, index], 0, pair_terms(1 + 2 * side, db, half))
            fin_copy[side, db, half] = remote(early.at[side, index], part(fin.at[side, db], half), ring_a(side), 'early')
        stage_next(index)
    for index in range(PIECES):
        for side in (0, 1):
            db, half = LATE[side][index]
            terms = pair_terms(1 + 2 * side, db, half)
            for other in (0, 1):
                raw_copy[side, other, index].wait_recv()
                terms.append((relay_raw.at[side, other, index], 0))
            add_half(late.at[side, index], 0, terms)
            fin_copy[side, db, half] = remote(late.at[side, index], part(fin.at[side, db], half), ring_a(side), 'late')
        if PIECES + index < len(STAGES):
            stage_next(PIECES + index)

    def first_sum(db, half):
        terms = pair_terms(0, db, half)
        for side in (0, 1):
            fin_copy[side, db, half].wait_recv()
            terms.append((fin.at[side, db], half * HALF))
        add_half(sums.at[db], half * HALF, terms)

    mid_copy = {}
    end_copy = {}
    for side in (0, 1):
        first_sum(2, side)
        mid_copy[side] = remote(part(sums.at[2], side), mid.at[side], ring_b(side), 'mid')
    for side in (0, 1):
        db, half = 1 + 2 * side, 1 - side
        first_sum(db, half)
        end_copy[side, half] = remote(part(sums.at[db], half), part(end.at[side], half), ring_b(side), 'end')
    for side in (0, 1):
        first_sum(1 + 2 * side, side)
    for side in (0, 1):
        db = 1 + 2 * side
        mid_copy[side].wait_recv()
        add_half(sums.at[db], side * HALF, [(sums.at[db], side * HALF), (mid.at[side], 0)])
        end_copy[side, side] = remote(part(sums.at[db], side), part(end.at[side], side), ring_b(side), 'end')
    ahead_copy = {}
    for side in (0, 1):
        ahead_copy[2, side] = remote(part(master, 0), part(ahead_weight.at[side], 0), ring_b(side), 'weight')
    for side in (0, 1):
        first_sum(0, side)
    for side in (0, 1):
        end_copy[side, 1 - side].wait_recv()
    for side in (0, 1):
        end_copy[side, side].wait_recv()

    def gather_sum(offset, carry):
        for tile in range(TILES):
            total = sums[0, tile, :, at(offset)] + end[0, tile, :, at(offset)] + end[1, tile, :, at(offset)]
            grad_sum[tile, :, at(offset)] = total
            carry = carry + total * total
        return carry

    mine_index = (x * 4 + z) * 8 + y * 2 + core
    sum_sent = []

    def global_sum(which, value, source, target):
        rows[which] = value
        slots[which, mine_index] = value
        for offsets in EVERY:
            pltpu.make_async_remote_copy(src_ref=rows.at[which], dst_ref=slots.at[which, mine_index], send_sem=sum_send.at[which], recv_sem=sum_recv.at[which], device_id=peer(*offsets), device_id_type=MESH).start()
        for side in (0, 1):
            ahead_copy[which, side] = remote(source, target(side), ring_b(side), AHEAD[which])
        block = slots.at[which, pl.ds(0, len(EVERY))]
        total = pltpu.make_async_remote_copy(src_ref=block, dst_ref=block, send_sem=sum_send.at[which], recv_sem=sum_recv.at[which], device_id=partner, device_id_type=MESH)
        total.wait_recv()
        sum_sent.append(total)
        received = [slots[which, slot] for slot in range(DEVICES)]
        while len(received) > 1:
            received = [left + right for left, right in zip(received[::2], received[1::2])]
        return received[0]

    grad_sq = global_sum(0, jnp.sum(fold(columns_loop(gather_sum, zero)), axis=0, keepdims=True), part(master, 1), lambda side: part(ahead_weight.at[side], 1))
    norm_sq = jnp.sum(grad_sq, axis=1, keepdims=True) / (REPLICAS * REPLICAS)
    clip = jnp.minimum(1.0, MAX_NORM / jnp.sqrt(norm_sq)) / REPLICAS

    def moments(offset, carry):
        squares = []
        for tile in range(TILES):
            scaled = clip * grad_sum[tile, :, at(offset)]
            new_one = BETA_ONE * one[tile, :, at(offset)] + (1.0 - BETA_ONE) * scaled
            new_two = BETA_TWO * two[tile, :, at(offset)] + (1.0 - BETA_TWO) * scaled * scaled
            step = (new_one * (1.0 / CORR_ONE)) / (jnp.sqrt(new_two * (1.0 / CORR_TWO)) + EPSILON) + WEIGHT_DECAY * master[tile, :, at(offset)]
            one_out[tile, :, at(offset)] = new_one
            two_out[tile, :, at(offset)] = new_two
            direction[tile, :, at(offset)] = step
            squares.append(carry[tile] + step * step)
        return tuple(squares)

    step_sq = [jnp.sum(fold(value), axis=1, keepdims=True) for value in columns_loop(moments, (zero,) * TILES)]

    lane = lax.broadcasted_iota(jnp.int32, (8, 128), 1)
    sub = lax.broadcasted_iota(jnp.int32, (8, 128), 0)
    spread_sums = jnp.zeros((8, 128), jnp.float32)
    for tile in range(TILES):
        spread_sums = jnp.where(lane == 8 * tile + sub, step_sq[tile], spread_sums)
        spread_sums = jnp.where(lane == 32 + 8 * tile + sub, weight_sq[tile], spread_sums)

    def tensor_of(row):
        layer = jnp.where(row >= 12, 1, 0)
        block = row - 12 * layer
        return 4 * layer + jnp.where(block >= 3, 1, 0) + jnp.where(block >= 4, 1, 0) + jnp.where(block >= 8, 1, 0)

    row_sums = jnp.broadcast_to(global_sum(1, jnp.sum(spread_sums, axis=0, keepdims=True), direction, lambda side: ahead_step.at[side]), (8, 128))
    rate = []
    for tile in range(TILES):
        tensor = tensor_of(8 * tile + sub)
        step_mask = (tensor_of(lane) == tensor) & (lane < 24)
        weight_mask = (tensor_of(lane - 32) == tensor) & (lane >= 32) & (lane < 56)
        step_norm = jnp.sqrt(jnp.sum(jnp.where(step_mask, row_sums, 0.0), axis=1, keepdims=True))
        weight_norm = jnp.sqrt(jnp.sum(jnp.where(weight_mask, row_sums, 0.0), axis=1, keepdims=True))
        rate.append(LEARN_RATE * (weight_norm / step_norm))

    def weights(db, weight, step, master_new=None):
        start = column(0, db)

        def body(offset, carry):
            for tile in range(TILES):
                value = weight[tile, :, at(offset)] - rate[tile] * step[tile, :, at(offset)]
                if master_new is not None:
                    master_new[tile, :, at(offset)] = value
                params[tile, :, at(start + offset)] = value.astype(jnp.bfloat16)
            return carry

        columns_loop(body)

    handed = []
    hand_sem = hand_sems.at[0]
    along_a = {}
    far_b = {}
    far_a = {}

    def send(da, db, half, device):
        ref = piece(params, da, db, half)
        return remote(ref, ref, device)

    def give(ref, device):
        handed.append(ref.shape[-1])
        remote(ref, ref, device, 'gather', hand_sem)

    def hand(da, db, half):
        give(piece(params, da, db, half), partner)

    def pass_on(first, second):
        for one_piece, other_piece in ((first, second), (second, first)):
            along_a[0, one_piece] = send(0, *one_piece, ring_a(0))
            along_a[1, other_piece] = send(0, *other_piece, ring_a(1))

    def quarter(da, half, index):
        start = column(da, 2) + half * HALF + index * QUARTER
        return params.at[:, :, pl.ds(pl.multiple_of(start, QUARTER), QUARTER)]

    def arrived(side, db, half):
        along_a[side, (db, half)].wait_recv()
        da = 3 - 2 * side
        if half == side and db == 2:
            first, second = quarter(da, half, 0), quarter(da, half, 1)
            far_a[db, half] = remote(first, first, ring_a(side))
            give(second, ring_a(side))
            give(second, peer(0, (1 - 2 * side) * core, (1 - 2 * side) * (1 - core), 1))
        elif half == side:
            far_a[db, half] = send(da, db, half, ring_a(side))
        hand(da, db, half)

    weights(0, master, direction, master_out)
    pass_on((0, 0), (0, 1))
    hand(0, 0, 0)
    hand(0, 0, 1)
    for side in (0, 1):
        db = 3 - 2 * side
        for which in (2, 0, 1):
            ahead_copy[which, side].wait_recv()
        weights(db, ahead_weight.at[side], ahead_step.at[side])
        far_b[side] = send(0, db, side, ring_b(side))
    pass_on((3, 0), (1, 1))
    pass_on((1, 0), (3, 1))
    for half in (0, 1):
        hand(0, 3, half)
        hand(0, 1, 1 - half)
    for side in (0, 1):
        arrived(side, 0, side)
    for side in (0, 1):
        far_b[side].wait_recv()
    pass_on((2, 0), (2, 1))
    hand(0, 2, 0)
    hand(0, 2, 1)
    for ref, group in ((relay_raw, 'raw'), (pair_raw, 'pair'), (early, 'early'), (late, 'late'), (mid, 'mid'), (end, 'end'), (ahead_weight, 'weight'), (ahead_step, 'step')):
        all_of(ref, group).wait_send()
    for copy in sum_sent:
        copy.wait_send()
    for side in (0, 1):
        arrived(side, 0, 1 - side)
    for pieces in (((3, 0), (1, 1)), ((1, 1), (3, 0)), ((1, 0), (3, 1)), ((3, 1), (1, 0)), ((2, 0), (2, 1)), ((2, 1), (2, 0))):
        for side in (0, 1):
            arrived(side, *pieces[side])
    for db in (0, 3, 1, 2):
        for half in (0, 1):
            far_a[db, half].wait_recv()
            if db == 2:
                give(quarter(2, half, 0), partner)
            else:
                hand(2, db, half)
    if len(started) != COPIES:
        raise ValueError(len(started))
    all_of(params.at[:, :, pl.ds(0, sum(handed))], landing=hand_sem).wait_recv()
    all_of(params.at[:, :, pl.ds(0, sum(gathered))]).wait_send()


def write_kernel(params, master, one, two, params_out, master_out, one_out, two_out, sem):
    pairs = [(master, master_out), (one, one_out), (two, two_out)]
    width = params.shape[2] // WRITE_PIECES
    for tile in range(TILES):
        for index in range(WRITE_PIECES):
            cols = pl.ds(index * width, width)
            pairs.append((params.at[tile, :, cols], params_out.at[tile, :, cols]))
    copies = [pltpu.make_async_copy(src, dst, sem.at[index]) for index, (src, dst) in enumerate(pairs)]
    for copy in copies:
        copy.start()
    for copy in copies:
        copy.wait()


def solution(mesh):
    state_spec = P(None, ('model', 'data'))

    def device_step(local_grads, master, moment_one, moment_two):
        state = (TILES, 8, SLAB)
        width = local_grads.shape[2]
        hbm = pl.BlockSpec(memory_space=pltpu.HBM)
        vmem = pl.BlockSpec(memory_space=pltpu.VMEM)

        def slabs(count, dtype, length=SLAB):
            return pltpu.VMEM(count + (TILES, 8, length), dtype)

        operands = (local_grads.reshape(TILES, 8, width), master.reshape(state), moment_one.reshape(state), moment_two.reshape(state))
        results = pl.pallas_call(
            lamb_kernel,
            name='lamb_step',
            out_shape=(
                pltpu.VMEM((TILES, 8, width), jnp.bfloat16),
                pltpu.VMEM(state, jnp.float32),
                pltpu.VMEM(state, jnp.float32),
                pltpu.VMEM(state, jnp.float32),
            ),
            in_specs=[hbm] * 4,
            out_specs=(vmem,) * 4,
            scratch_shapes=[
                slabs((len(ORDER),), jnp.bfloat16),
                slabs((len(ORDER),), jnp.bfloat16),
                slabs((2, 2, PIECES), jnp.bfloat16, HALF),
                slabs((2, PIECES), jnp.float32, HALF),
                slabs((2, PIECES), jnp.float32, HALF),
                slabs((2, 4), jnp.float32),
                slabs((4,), jnp.float32),
                slabs((2,), jnp.float32, HALF),
                slabs((2,), jnp.float32),
                slabs((), jnp.float32),
                slabs((), jnp.float32),
                slabs((), jnp.float32),
                slabs((), jnp.float32),
                slabs((), jnp.float32),
                slabs((2,), jnp.float32),
                slabs((2,), jnp.float32),
                pltpu.VMEM((2, 1, 128), jnp.float32),
                pltpu.VMEM((2, DEVICES, 1, 128), jnp.float32),
                pltpu.SemaphoreType.DMA((len(GROUPS),)),
                pltpu.SemaphoreType.DMA((COPIES,)),
                pltpu.SemaphoreType.DMA((LOADS,)),
                pltpu.SemaphoreType.DMA((2,)),
                pltpu.SemaphoreType.DMA((2,)),
                pltpu.SemaphoreType.DMA((1,)),
                pltpu.SemaphoreType.REGULAR((len(STAGES),)),
            ],
            compiler_params=pltpu.CompilerParams(collective_id=0, has_side_effects=True, vmem_limit_bytes=VMEM_LIMIT),
        )(*(pltpu.with_memory_space_constraint(operand, pltpu.HBM) for operand in operands))
        outs = pl.pallas_call(
            write_kernel,
            name='write_out',
            out_shape=tuple(pltpu.HBM(result.shape, result.dtype) for result in results),
            in_specs=[vmem] * 4,
            out_specs=(hbm,) * 4,
            scratch_shapes=[pltpu.SemaphoreType.DMA((TILES * WRITE_PIECES + 3,))],
            compiler_params=pltpu.CompilerParams(vmem_limit_bytes=2 ** 20),
        )(*results)
        return tuple(out.reshape(24, -1) for out in outs)

    return jax.shard_map(device_step, mesh=mesh, in_specs=(P('data', None, 'model'), state_spec, state_spec, state_spec), out_specs=(P(None, 'model'), state_spec, state_spec, state_spec), check_vma=False)
```

```python
import functools

import jax
import jax.numpy as jnp
from jax import lax
from jax.experimental import pallas as pl
from jax.experimental.pallas import tpu as pltpu
from jax.sharding import PartitionSpec as P

STEP = 4
LEARN_RATE = 0.08
BETA_ONE = 0.9
BETA_TWO = 0.999
EPSILON = 1e-6
WEIGHT_DECAY = 0.01
MAX_NORM = 1.0
CORR_ONE = 1.0 - BETA_ONE ** STEP
CORR_TWO = 1.0 - BETA_TWO ** STEP

MESH = pl.DeviceIdType.MESH
TILES = 3
SLAB = 4608
HALF = SLAB // 2
QUARTER = SLAB // 4
STEP_COLS = 768
REPLICAS = 32
LATE = (((2, 0), (1, 1), (1, 0), (0, 0)), ((2, 1), (3, 0), (3, 1), (0, 1)))
EARLY = (((3, 0), (3, 1), (2, 1), (0, 1)), ((1, 1), (1, 0), (2, 0), (0, 0)))
PIECES = 4
ORDER = ((1, 3), (3, 1), (1, 2), (3, 2), (1, 0), (3, 0), (1, 1), (3, 3), (0, 2), (0, 1), (0, 3), (0, 0))
EVERY = sorted(((i, j, k, e) for i in range(4) for j in range(4) for k in range(4) for e in range(2) if i + j + k + e), key=lambda far: -sum(min(step, 4 - step) for step in far[:3]) - far[3] / 2)
DEVICES = len(EVERY) + 1
ALONG_X = tuple((k, 0, 0, 0) for k in (1, 3))
ALONG_Z = tuple((0, k, 0, 0) for k in (1, 3))
ALONG_Y = tuple((0, 0, k, 0) for k in (1, 3))
OTHER_CORE = ((0, 0, 0, 1),)
BARRIER = ALONG_X + ALONG_Z + ALONG_Y + OTHER_CORE + tuple((0, k, 0, 1) for k in (1, 3)) + tuple((0, 0, k, 1) for k in (1, 3))
STAGES = (ALONG_X, OTHER_CORE, ALONG_Y, ALONG_Y, ALONG_Z, ALONG_Z)
GROUPS = ('raw', 'pair', 'early', 'late', 'mid', 'end', 'weight', 'step', 'gather')
AHEAD = ('weight', 'step')
COPIES = 36
BATCH = 4
VMEM_LIMIT = 40 * 2 ** 20
WRITE_PIECES = 4


def lamb_kernel(grads, master_in, one_in, two_in, params, master_out, one_out, two_out, own_raw, pair_raw, relay_raw, early, late, fin, sums, mid, end, state, grad_sum, direction, ahead_weight, ahead_step, rows, slots, send_sem, recv_sem, sum_send, sum_recv, group_sem, raw_sem, pair_sem, ahead_sem, stage_sem):
    x, data = lax.axis_index('model'), lax.axis_index('data')
    core, y, z = lax.rem(data, 2), lax.rem(data // 2, 4), data // 8
    started = []
    gathered = []
    hand_sem, own_sem, state_sem, early_sem, end_sem = (group_sem.at[index] for index in range(5))

    def peer(dx, dz, dy, dc):
        chip = lax.rem(z + dz + 4, 4) * 4 + lax.rem(y + dy + 4, 4)
        return lax.rem(x + dx, 4), chip * 2 + lax.rem(core + dc, 2)

    def ring_a(side, other=0):
        role = core if not other else 1 - core
        step = 1 - 2 * side
        return peer(0, step * role, step * (1 - role), other)

    def ring_b(side):
        step = 1 - 2 * side
        return peer(0, step * (1 - core), step * core, 0)

    partner = peer(0, 0, 0, 1)

    def column(da, db, other=0):
        role = core if not other else 1 - core
        dy, dz = da * (1 - role) + db * role, da * role + db * (1 - role)
        slab = (lax.rem(z + dz, 4) * 4 + lax.rem(y + dy, 4)) * 2 + role
        return pl.multiple_of(slab * SLAB, SLAB)

    def whole(ref, da, db, other=0):
        return ref.at[:, :, pl.ds(column(da, db, other), SLAB)]

    def piece(ref, da, db, half, other=0):
        return ref.at[:, :, pl.ds(pl.multiple_of(column(da, db, other) + half * HALF, HALF), HALF)]

    def part(ref, half):
        return ref.at[:, :, pl.ds(half * HALF, HALF)]

    def remote(src, dst, device, group='gather', landing=None):
        if landing is None:
            landing = recv_sem.at[len(started)]
            started.append(group)
        if group == 'gather':
            gathered.append(src.shape[-1])
        copy = pltpu.make_async_remote_copy(src_ref=src, dst_ref=dst, send_sem=send_sem.at[GROUPS.index(group)], recv_sem=landing, device_id=device, device_id_type=MESH)
        copy.start()
        return copy

    def all_of(ref, group='gather', landing=None):
        landing = recv_sem.at[0] if landing is None else landing
        return pltpu.make_async_remote_copy(src_ref=ref, dst_ref=ref, send_sem=send_sem.at[GROUPS.index(group)], recv_sem=landing, device_id=partner, device_id_type=MESH)

    def load(src, dst, sem):
        pltpu.make_async_copy(src, dst, sem).start()

    def columns_loop(body, init=0, length=SLAB):
        def step(index, carry):
            return body(index * STEP_COLS, carry)
        return lax.fori_loop(0, length // STEP_COLS, step, init)

    def at(start):
        return pl.ds(pl.multiple_of(start, 128), STEP_COLS)

    def add_half(target, target_start, terms):
        def body(offset, carry):
            for tile in range(TILES):
                total = None
                for term, start in terms:
                    value = term[tile, :, at(start + offset)].astype(jnp.float32)
                    total = value if total is None else total + value
                target[tile, :, at(target_start + offset)] = total
            return carry
        columns_loop(body, 0, HALF)

    barrier = pltpu.get_barrier_semaphore()
    for offsets in BARRIER:
        pl.semaphore_signal(barrier, inc=1, device_id=peer(*offsets), device_id_type=MESH)

    def stage_signal(stage):
        for offsets in STAGES[stage]:
            pl.semaphore_signal(stage_sem.at[stage], inc=1, device_id=peer(*offsets), device_id_type=MESH)

    def stage_next(stage):
        pl.semaphore_wait(stage_sem.at[stage], len(STAGES[stage]))
        if stage + 1 < len(STAGES):
            stage_signal(stage + 1)

    place = {key: index for index, key in enumerate(ORDER)}
    for key in ORDER:
        load(whole(grads, *key), own_raw.at[place[key]], own_sem)
    for index, source in enumerate((master_in, one_in, two_in)):
        load(source, state.at[index], state_sem)
    master, one, two = (state.at[index] for index in range(3))

    pl.semaphore_wait(barrier, len(BARRIER))

    for index in range(PIECES):
        for side in (0, 1):
            for other in (0, 1):
                db, half = LATE[side][index]
                remote(piece(grads, 2, db, half, other), relay_raw.at[side, other, index], ring_a(side, other), 'raw', raw_sem.at[side, index])
    for key in ORDER:
        remote(whole(grads, *key, other=1), pair_raw.at[place[key]], partner, 'pair', pair_sem.at[place[key] // BATCH])

    stage_signal(0)

    def fold(value):
        parts = [value[:, 128 * k:128 * (k + 1)] for k in range(STEP_COLS // 128)]
        while len(parts) > 1:
            parts = [left + right for left, right in zip(parts[::2], parts[1::2])] + parts[len(parts) - len(parts) % 2:]
        return parts[0]

    def weight_square(offset, carry):
        return tuple(carry[tile] + master[tile, :, at(offset)] * master[tile, :, at(offset)] for tile in range(TILES))

    pltpu.make_async_copy(state, state, state_sem).wait()
    zero = jnp.zeros((8, STEP_COLS), jnp.float32)
    weight_sq = [jnp.sum(fold(value), axis=1, keepdims=True) for value in columns_loop(weight_square, (zero,) * TILES)]

    ready = set()

    def pair_terms(da, db, half):
        slot = place[da, db]
        batch = slot // BATCH
        if not ready:
            pltpu.make_async_copy(own_raw, own_raw, own_sem).wait()
        if batch not in ready:
            all_of(pair_raw.at[pl.ds(batch * BATCH, BATCH)], 'pair', pair_sem.at[batch]).wait_recv()
            ready.add(batch)
        return [(own_raw.at[slot], half * HALF), (pair_raw.at[slot], half * HALF)]

    fin_copy = {}
    for index in range(PIECES):
        for side in (0, 1):
            db, half = EARLY[side][index]
            add_half(early.at[side, index], 0, pair_terms(1 + 2 * side, db, half))
            remote(early.at[side, index], part(fin.at[side, db], half), ring_a(side), 'early', early_sem)
        stage_next(index)
    for index in range(PIECES):
        for side in (0, 1):
            db, half = LATE[side][index]
            terms = pair_terms(1 + 2 * side, db, half)
            all_of(relay_raw.at[side, pl.ds(0, 2), index], 'raw', raw_sem.at[side, index]).wait_recv()
            terms += [(relay_raw.at[side, other, index], 0) for other in (0, 1)]
            add_half(late.at[side, index], 0, terms)
            fin_copy[side, db, half] = remote(late.at[side, index], part(fin.at[side, db], half), ring_a(side), 'late')
        if PIECES + index < len(STAGES):
            stage_next(PIECES + index)

    arrived_early = []

    def first_sum(db, half):
        terms = pair_terms(0, db, half)
        if not arrived_early:
            all_of(early, 'early', early_sem).wait_recv()
            arrived_early.append(db)
        for side in (0, 1):
            if (side, db, half) in fin_copy:
                fin_copy[side, db, half].wait_recv()
            terms.append((fin.at[side, db], half * HALF))
        add_half(sums.at[db], half * HALF, terms)

    mid_copy = {}
    for side in (0, 1):
        first_sum(2, side)
        mid_copy[side] = remote(part(sums.at[2], side), mid.at[side], ring_b(side), 'mid')
    for side in (0, 1):
        db, half = 1 + 2 * side, 1 - side
        first_sum(db, half)
        remote(part(sums.at[db], half), part(end.at[side], half), ring_b(side), 'end', end_sem)
    for side in (0, 1):
        first_sum(1 + 2 * side, side)
    for side in (0, 1):
        db = 1 + 2 * side
        mid_copy[side].wait_recv()
        add_half(sums.at[db], side * HALF, [(sums.at[db], side * HALF), (mid.at[side], 0)])
        remote(part(sums.at[db], side), part(end.at[side], side), ring_b(side), 'end', end_sem)
    for side in (0, 1):
        remote(part(master, 0), part(ahead_weight.at[side], 0), ring_b(side), 'weight', ahead_sem.at[0])
    for side in (0, 1):
        first_sum(0, side)
    all_of(end, 'end', end_sem).wait_recv()

    def gather_sum(offset, carry):
        for tile in range(TILES):
            total = sums[0, tile, :, at(offset)] + end[0, tile, :, at(offset)] + end[1, tile, :, at(offset)]
            grad_sum[tile, :, at(offset)] = total
            carry = carry + total * total
        return carry

    mine_index = (x * 4 + z) * 8 + y * 2 + core
    sum_sent = []

    def global_sum(which, value, source, target):
        rows[which] = value
        slots[which, mine_index] = value
        for offsets in EVERY:
            pltpu.make_async_remote_copy(src_ref=rows.at[which], dst_ref=slots.at[which, mine_index], send_sem=sum_send.at[which], recv_sem=sum_recv.at[which], device_id=peer(*offsets), device_id_type=MESH).start()
        for side in (0, 1):
            remote(source, target(side), ring_b(side), AHEAD[which], ahead_sem.at[which])
        block = slots.at[which, pl.ds(0, len(EVERY))]
        total = pltpu.make_async_remote_copy(src_ref=block, dst_ref=block, send_sem=sum_send.at[which], recv_sem=sum_recv.at[which], device_id=partner, device_id_type=MESH)
        total.wait_recv()
        sum_sent.append(total)
        received = [slots[which, slot] for slot in range(DEVICES)]
        while len(received) > 1:
            received = [left + right for left, right in zip(received[::2], received[1::2])]
        return received[0]

    grad_sq = global_sum(0, jnp.sum(fold(columns_loop(gather_sum, zero)), axis=0, keepdims=True), part(master, 1), lambda side: part(ahead_weight.at[side], 1))
    norm_sq = jnp.sum(grad_sq, axis=1, keepdims=True) / (REPLICAS * REPLICAS)
    clip = jnp.minimum(1.0, MAX_NORM / jnp.sqrt(norm_sq)) / REPLICAS

    def moments(offset, carry):
        squares = []
        for tile in range(TILES):
            scaled = clip * grad_sum[tile, :, at(offset)]
            new_one = BETA_ONE * one[tile, :, at(offset)] + (1.0 - BETA_ONE) * scaled
            new_two = BETA_TWO * two[tile, :, at(offset)] + (1.0 - BETA_TWO) * scaled * scaled
            step = (new_one * (1.0 / CORR_ONE)) / (jnp.sqrt(new_two * (1.0 / CORR_TWO)) + EPSILON) + WEIGHT_DECAY * master[tile, :, at(offset)]
            one_out[tile, :, at(offset)] = new_one
            two_out[tile, :, at(offset)] = new_two
            direction[tile, :, at(offset)] = step
            squares.append(carry[tile] + step * step)
        return tuple(squares)

    step_sq = [jnp.sum(fold(value), axis=1, keepdims=True) for value in columns_loop(moments, (zero,) * TILES)]

    lane = lax.broadcasted_iota(jnp.int32, (8, 128), 1)
    sub = lax.broadcasted_iota(jnp.int32, (8, 128), 0)
    spread_sums = jnp.zeros((8, 128), jnp.float32)
    for tile in range(TILES):
        spread_sums = jnp.where(lane == 8 * tile + sub, step_sq[tile], spread_sums)
        spread_sums = jnp.where(lane == 32 + 8 * tile + sub, weight_sq[tile], spread_sums)

    def tensor_of(row):
        layer = jnp.where(row >= 12, 1, 0)
        block = row - 12 * layer
        return 4 * layer + jnp.where(block >= 3, 1, 0) + jnp.where(block >= 4, 1, 0) + jnp.where(block >= 8, 1, 0)

    row_sums = jnp.broadcast_to(global_sum(1, jnp.sum(spread_sums, axis=0, keepdims=True), direction, lambda side: ahead_step.at[side]), (8, 128))
    rate = []
    for tile in range(TILES):
        tensor = tensor_of(8 * tile + sub)
        step_mask = (tensor_of(lane) == tensor) & (lane < 24)
        weight_mask = (tensor_of(lane - 32) == tensor) & (lane >= 32) & (lane < 56)
        step_norm = jnp.sqrt(jnp.sum(jnp.where(step_mask, row_sums, 0.0), axis=1, keepdims=True))
        weight_norm = jnp.sqrt(jnp.sum(jnp.where(weight_mask, row_sums, 0.0), axis=1, keepdims=True))
        rate.append(LEARN_RATE * (weight_norm / step_norm))

    def weights(db, weight, step, master_new=None):
        start = column(0, db)

        def body(offset, carry):
            for tile in range(TILES):
                value = weight[tile, :, at(offset)] - rate[tile] * step[tile, :, at(offset)]
                if master_new is not None:
                    master_new[tile, :, at(offset)] = value
                params[tile, :, at(start + offset)] = value.astype(jnp.bfloat16)
            return carry

        columns_loop(body)

    handed = []
    along_a = {}
    far_b = {}
    far_a = {}

    def send(da, db, half, device):
        ref = piece(params, da, db, half)
        return remote(ref, ref, device)

    def give(ref, device):
        handed.append(ref.shape[-1])
        remote(ref, ref, device, 'gather', hand_sem)

    def hand(da, db, half):
        give(piece(params, da, db, half), partner)

    def pass_on(first, second):
        for one_piece, other_piece in ((first, second), (second, first)):
            along_a[0, one_piece] = send(0, *one_piece, ring_a(0))
            along_a[1, other_piece] = send(0, *other_piece, ring_a(1))

    def quarter(da, half, index):
        start = column(da, 2) + half * HALF + index * QUARTER
        return params.at[:, :, pl.ds(pl.multiple_of(start, QUARTER), QUARTER)]

    def arrived(side, db, half):
        along_a[side, (db, half)].wait_recv()
        da = 3 - 2 * side
        if half == side and db == 2:
            first, second = quarter(da, half, 0), quarter(da, half, 1)
            far_a[db, half] = remote(first, first, ring_a(side))
            give(second, ring_a(side))
            give(second, peer(0, (1 - 2 * side) * core, (1 - 2 * side) * (1 - core), 1))
        elif half == side:
            far_a[db, half] = send(da, db, half, ring_a(side))
        hand(da, db, half)

    weights(0, master, direction, master_out)
    pass_on((0, 0), (0, 1))
    hand(0, 0, 0)
    hand(0, 0, 1)
    all_of(ahead_weight, 'weight', ahead_sem.at[0]).wait_recv()
    all_of(ahead_step, 'step', ahead_sem.at[1]).wait_recv()
    for side in (0, 1):
        db = 3 - 2 * side
        weights(db, ahead_weight.at[side], ahead_step.at[side])
        far_b[side] = send(0, db, side, ring_b(side))
    pass_on((3, 0), (1, 1))
    pass_on((1, 0), (3, 1))
    for half in (0, 1):
        hand(0, 3, half)
        hand(0, 1, 1 - half)
    for side in (0, 1):
        arrived(side, 0, side)
    for side in (0, 1):
        far_b[side].wait_recv()
    pass_on((2, 0), (2, 1))
    hand(0, 2, 0)
    hand(0, 2, 1)
    for ref, group in ((relay_raw, 'raw'), (pair_raw, 'pair'), (early, 'early'), (late, 'late'), (mid, 'mid'), (end, 'end'), (ahead_weight, 'weight'), (ahead_step, 'step')):
        all_of(ref, group).wait_send()
    for copy in sum_sent:
        copy.wait_send()
    for side in (0, 1):
        arrived(side, 0, 1 - side)
    for pieces in (((3, 0), (1, 1)), ((1, 1), (3, 0)), ((1, 0), (3, 1)), ((3, 1), (1, 0)), ((2, 0), (2, 1)), ((2, 1), (2, 0))):
        for side in (0, 1):
            arrived(side, *pieces[side])
    for db in (0, 3, 1, 2):
        for half in (0, 1):
            far_a[db, half].wait_recv()
            if db == 2:
                give(quarter(2, half, 0), partner)
            else:
                hand(2, db, half)
    if len(started) != COPIES:
        raise ValueError(len(started))
    all_of(params.at[:, :, pl.ds(0, sum(handed))], landing=hand_sem).wait_recv()
    all_of(params.at[:, :, pl.ds(0, sum(gathered))]).wait_send()


def write_kernel(params, master, one, two, params_out, master_out, one_out, two_out, sem):
    pairs = [(master, master_out), (one, one_out), (two, two_out)]
    width = params.shape[2] // WRITE_PIECES
    for tile in range(TILES):
        for index in range(WRITE_PIECES):
            cols = pl.ds(index * width, width)
            pltpu.make_async_copy(params.at[tile, :, cols], params_out.at[tile, :, cols], sem.at[0]).start()
    copies = [pltpu.make_async_copy(src, dst, sem.at[1 + index]) for index, (src, dst) in enumerate(pairs)]
    for copy in copies:
        copy.start()
    for copy in copies:
        copy.wait()
    pltpu.make_async_copy(params, params_out, sem.at[0]).wait()


def solution(mesh):
    state_spec = P(None, ('model', 'data'))

    def device_step(local_grads, master, moment_one, moment_two):
        state = (TILES, 8, SLAB)
        width = local_grads.shape[2]
        hbm = pl.BlockSpec(memory_space=pltpu.HBM)
        vmem = pl.BlockSpec(memory_space=pltpu.VMEM)

        def slabs(count, dtype, length=SLAB):
            return pltpu.VMEM(count + (TILES, 8, length), dtype)

        operands = (local_grads.reshape(TILES, 8, width), master.reshape(state), moment_one.reshape(state), moment_two.reshape(state))
        results = pl.pallas_call(
            lamb_kernel,
            name='lamb_step',
            out_shape=(
                pltpu.VMEM((TILES, 8, width), jnp.bfloat16),
                pltpu.VMEM(state, jnp.float32),
                pltpu.VMEM(state, jnp.float32),
                pltpu.VMEM(state, jnp.float32),
            ),
            in_specs=[hbm] * 4,
            out_specs=(vmem,) * 4,
            scratch_shapes=[
                slabs((len(ORDER),), jnp.bfloat16),
                slabs((len(ORDER),), jnp.bfloat16),
                slabs((2, 2, PIECES), jnp.bfloat16, HALF),
                slabs((2, PIECES), jnp.float32, HALF),
                slabs((2, PIECES), jnp.float32, HALF),
                slabs((2, 4), jnp.float32),
                slabs((4,), jnp.float32),
                slabs((2,), jnp.float32, HALF),
                slabs((2,), jnp.float32),
                slabs((3,), jnp.float32),
                slabs((), jnp.float32),
                slabs((), jnp.float32),
                slabs((2,), jnp.float32),
                slabs((2,), jnp.float32),
                pltpu.VMEM((2, 1, 128), jnp.float32),
                pltpu.VMEM((2, DEVICES, 1, 128), jnp.float32),
                pltpu.SemaphoreType.DMA((len(GROUPS),)),
                pltpu.SemaphoreType.DMA((COPIES,)),
                pltpu.SemaphoreType.DMA((2,)),
                pltpu.SemaphoreType.DMA((2,)),
                pltpu.SemaphoreType.DMA((5,)),
                pltpu.SemaphoreType.DMA((2, PIECES)),
                pltpu.SemaphoreType.DMA((len(ORDER) // BATCH,)),
                pltpu.SemaphoreType.DMA((2,)),
                pltpu.SemaphoreType.REGULAR((len(STAGES),)),
            ],
            compiler_params=pltpu.CompilerParams(collective_id=0, has_side_effects=True, vmem_limit_bytes=VMEM_LIMIT),
        )(*(pltpu.with_memory_space_constraint(operand, pltpu.HBM) for operand in operands))
        outs = pl.pallas_call(
            write_kernel,
            name='write_out',
            out_shape=tuple(pltpu.HBM(result.shape, result.dtype) for result in results),
            in_specs=[vmem] * 4,
            out_specs=(hbm,) * 4,
            scratch_shapes=[pltpu.SemaphoreType.DMA((4,))],
            compiler_params=pltpu.CompilerParams(vmem_limit_bytes=2 ** 20),
        )(*results)
        return tuple(out.reshape(24, -1) for out in outs)

    return jax.shard_map(device_step, mesh=mesh, in_specs=(P('data', None, 'model'), state_spec, state_spec, state_spec), out_specs=(P(None, 'model'), state_spec, state_spec, state_spec), check_vma=False)
```

```python
import functools

import jax
import jax.numpy as jnp
from jax import lax
from jax.experimental import pallas as pl
from jax.experimental.pallas import tpu as pltpu
from jax.sharding import PartitionSpec as P

STEP = 4
LEARN_RATE = 0.08
BETA_ONE = 0.9
BETA_TWO = 0.999
EPSILON = 1e-6
WEIGHT_DECAY = 0.01
MAX_NORM = 1.0
CORR_ONE = 1.0 - BETA_ONE ** STEP
CORR_TWO = 1.0 - BETA_TWO ** STEP

MESH = pl.DeviceIdType.MESH
TILES = 3
SLAB = 4608
HALF = SLAB // 2
QUARTER = SLAB // 4
STEP_COLS = 768
REPLICAS = 32
LATE = (((2, 0), (1, 1), (1, 0), (0, 0)), ((2, 1), (3, 0), (3, 1), (0, 1)))
EARLY = (((3, 0), (3, 1), (2, 1), (0, 1)), ((1, 1), (1, 0), (2, 0), (0, 0)))
PIECES = 4
ORDER = ((1, 3), (3, 1), (1, 2), (3, 2), (1, 0), (3, 0), (1, 1), (3, 3), (0, 2), (0, 1), (0, 3), (0, 0))
EVERY = sorted(((i, j, k, e) for i in range(4) for j in range(4) for k in range(4) for e in range(2) if i + j + k + e), key=lambda far: -sum(min(step, 4 - step) for step in far[:3]) - far[3] / 2)
DEVICES = len(EVERY) + 1
ALONG_X = tuple((k, 0, 0, 0) for k in (1, 3))
ALONG_Z = tuple((0, k, 0, 0) for k in (1, 3))
ALONG_Y = tuple((0, 0, k, 0) for k in (1, 3))
OTHER_CORE = ((0, 0, 0, 1),)
BARRIER = ALONG_X + ALONG_Z + ALONG_Y + OTHER_CORE + tuple((0, k, 0, 1) for k in (1, 3)) + tuple((0, 0, k, 1) for k in (1, 3))
STAGES = (ALONG_X, OTHER_CORE, ALONG_Y, ALONG_Y, ALONG_Z, ALONG_Z)
GROUPS = ('raw', 'pair', 'early', 'late', 'mid', 'end', 'weight', 'step', 'gather')
COPIES = 38
BATCH = 4
VMEM_LIMIT = 40 * 2 ** 20
WRITE_PIECES = 2


def lamb_kernel(grads, master_in, one_in, two_in, params, master_out, one_out, two_out, own_raw, pair_raw, relay_raw, early, late, fin, sums, mid, end, state, grad_sum, direction, ahead_weight, ahead_step, rows, slots, send_sem, recv_sem, sum_send, sum_recv, group_sem, raw_sem, pair_sem, ahead_sem, stage_sem):
    x, data = lax.axis_index('model'), lax.axis_index('data')
    core, y, z = lax.rem(data, 2), lax.rem(data // 2, 4), data // 8
    started = []
    gathered = []
    hand_sem, own_sem, state_sem, early_sem, end_sem = (group_sem.at[index] for index in range(5))

    def peer(dx, dz, dy, dc):
        chip = lax.rem(z + dz + 4, 4) * 4 + lax.rem(y + dy + 4, 4)
        return lax.rem(x + dx, 4), chip * 2 + lax.rem(core + dc, 2)

    def ring_a(side, other=0):
        role = core if not other else 1 - core
        step = 1 - 2 * side
        return peer(0, step * role, step * (1 - role), other)

    def ring_b(side):
        step = 1 - 2 * side
        return peer(0, step * (1 - core), step * core, 0)

    partner = peer(0, 0, 0, 1)

    def column(da, db, other=0):
        role = core if not other else 1 - core
        dy, dz = da * (1 - role) + db * role, da * role + db * (1 - role)
        slab = (lax.rem(z + dz, 4) * 4 + lax.rem(y + dy, 4)) * 2 + role
        return pl.multiple_of(slab * SLAB, SLAB)

    def whole(ref, da, db, other=0):
        return ref.at[:, :, pl.ds(column(da, db, other), SLAB)]

    def piece(ref, da, db, half, other=0):
        return ref.at[:, :, pl.ds(pl.multiple_of(column(da, db, other) + half * HALF, HALF), HALF)]

    def part(ref, half):
        return ref.at[:, :, pl.ds(half * HALF, HALF)]

    def remote(src, dst, device, group='gather', landing=None):
        if landing is None:
            landing = recv_sem.at[len(started)]
            started.append(group)
        if group == 'gather':
            gathered.append(src.shape[-1])
        copy = pltpu.make_async_remote_copy(src_ref=src, dst_ref=dst, send_sem=send_sem.at[GROUPS.index(group)], recv_sem=landing, device_id=device, device_id_type=MESH)
        copy.start()
        return copy

    def all_of(ref, group='gather', landing=None):
        landing = recv_sem.at[0] if landing is None else landing
        return pltpu.make_async_remote_copy(src_ref=ref, dst_ref=ref, send_sem=send_sem.at[GROUPS.index(group)], recv_sem=landing, device_id=partner, device_id_type=MESH)

    def load(src, dst, sem):
        pltpu.make_async_copy(src, dst, sem).start()

    def columns_loop(body, init=0, length=SLAB):
        def step(index, carry):
            return body(index * STEP_COLS, carry)
        return lax.fori_loop(0, length // STEP_COLS, step, init)

    def at(start):
        return pl.ds(pl.multiple_of(start, 128), STEP_COLS)

    def add_half(target, target_start, terms):
        def body(offset, carry):
            for tile in range(TILES):
                total = None
                for term, start in terms:
                    value = term[tile, :, at(start + offset)].astype(jnp.float32)
                    total = value if total is None else total + value
                target[tile, :, at(target_start + offset)] = total
            return carry
        columns_loop(body, 0, HALF)

    barrier = pltpu.get_barrier_semaphore()
    for offsets in BARRIER:
        pl.semaphore_signal(barrier, inc=1, device_id=peer(*offsets), device_id_type=MESH)

    def stage_signal(stage):
        for offsets in STAGES[stage]:
            pl.semaphore_signal(stage_sem.at[stage], inc=1, device_id=peer(*offsets), device_id_type=MESH)

    def stage_next(stage):
        pl.semaphore_wait(stage_sem.at[stage], len(STAGES[stage]))
        if stage + 1 < len(STAGES):
            stage_signal(stage + 1)

    place = {key: index for index, key in enumerate(ORDER)}
    pl.semaphore_wait(barrier, len(BARRIER))

    for index in range(PIECES):
        for side in (0, 1):
            for other in (0, 1):
                db, half = LATE[side][index]
                remote(piece(grads, 2, db, half, other), relay_raw.at[side, other, index], ring_a(side, other), 'raw', raw_sem.at[side, index])
    for key in ORDER:
        remote(whole(grads, *key, other=1), pair_raw.at[place[key]], partner, 'pair', pair_sem.at[place[key] // BATCH])

    for key in ORDER:
        load(whole(grads, *key), own_raw.at[place[key]], own_sem)
    for index, source in enumerate((master_in, one_in, two_in)):
        load(source, state.at[index], state_sem)
    master, one, two = (state.at[index] for index in range(3))

    stage_signal(0)

    def fold(value):
        parts = [value[:, 128 * k:128 * (k + 1)] for k in range(STEP_COLS // 128)]
        while len(parts) > 1:
            parts = [left + right for left, right in zip(parts[::2], parts[1::2])] + parts[len(parts) - len(parts) % 2:]
        return parts[0]

    def weight_square(offset, carry):
        return tuple(carry[tile] + master[tile, :, at(offset)] * master[tile, :, at(offset)] for tile in range(TILES))

    pltpu.make_async_copy(state, state, state_sem).wait()
    zero = jnp.zeros((8, STEP_COLS), jnp.float32)
    weight_sq = [jnp.sum(fold(value), axis=1, keepdims=True) for value in columns_loop(weight_square, (zero,) * TILES)]

    ready = set()

    def pair_terms(da, db, half):
        slot = place[da, db]
        batch = slot // BATCH
        if not ready:
            pltpu.make_async_copy(own_raw, own_raw, own_sem).wait()
        if batch not in ready:
            all_of(pair_raw.at[pl.ds(batch * BATCH, BATCH)], 'pair', pair_sem.at[batch]).wait_recv()
            ready.add(batch)
        return [(own_raw.at[slot], half * HALF), (pair_raw.at[slot], half * HALF)]

    fin_copy = {}
    for index in range(PIECES):
        for side in (0, 1):
            db, half = EARLY[side][index]
            add_half(early.at[side, index], 0, pair_terms(1 + 2 * side, db, half))
            remote(early.at[side, index], part(fin.at[side, db], half), ring_a(side), 'early', early_sem)
        stage_next(index)
    for index in range(PIECES):
        for side in (0, 1):
            db, half = LATE[side][index]
            terms = pair_terms(1 + 2 * side, db, half)
            all_of(relay_raw.at[side, pl.ds(0, 2), index], 'raw', raw_sem.at[side, index]).wait_recv()
            terms += [(relay_raw.at[side, other, index], 0) for other in (0, 1)]
            add_half(late.at[side, index], 0, terms)
            fin_copy[side, db, half] = remote(late.at[side, index], part(fin.at[side, db], half), ring_a(side), 'late')
        if PIECES + index < len(STAGES):
            stage_next(PIECES + index)

    arrived_early = []

    def first_sum(db, half):
        terms = pair_terms(0, db, half)
        if not arrived_early:
            all_of(early, 'early', early_sem).wait_recv()
            arrived_early.append(db)
        for side in (0, 1):
            if (side, db, half) in fin_copy:
                fin_copy[side, db, half].wait_recv()
            terms.append((fin.at[side, db], half * HALF))
        add_half(sums.at[db], half * HALF, terms)

    mid_copy = {}
    for side in (0, 1):
        first_sum(2, side)
        mid_copy[side] = remote(part(sums.at[2], side), mid.at[side], ring_b(side), 'mid')
    for side in (0, 1):
        db, half = 1 + 2 * side, 1 - side
        first_sum(db, half)
        remote(part(sums.at[db], half), part(end.at[side], half), ring_b(side), 'end', end_sem)
    for side in (0, 1):
        first_sum(1 + 2 * side, side)
    for side in (0, 1):
        db = 1 + 2 * side
        mid_copy[side].wait_recv()
        add_half(sums.at[db], side * HALF, [(sums.at[db], side * HALF), (mid.at[side], 0)])
        remote(part(sums.at[db], side), part(end.at[side], side), ring_b(side), 'end', end_sem)
    for side in (0, 1):
        remote(part(master, side), part(ahead_weight.at[side], side), ring_b(side), 'weight', ahead_sem.at[0])
    for side in (0, 1):
        first_sum(0, side)
    all_of(end, 'end', end_sem).wait_recv()

    def gather_sum(offset, carry):
        for tile in range(TILES):
            total = sums[0, tile, :, at(offset)] + end[0, tile, :, at(offset)] + end[1, tile, :, at(offset)]
            grad_sum[tile, :, at(offset)] = total
            carry = carry + total * total
        return carry

    mine_index = (x * 4 + z) * 8 + y * 2 + core
    sum_sent = []

    def global_sum(which, value, meanwhile=None):
        rows[which] = value
        slots[which, mine_index] = value
        for offsets in EVERY:
            pltpu.make_async_remote_copy(src_ref=rows.at[which], dst_ref=slots.at[which, mine_index], send_sem=sum_send.at[which], recv_sem=sum_recv.at[which], device_id=peer(*offsets), device_id_type=MESH).start()
        if meanwhile is not None:
            meanwhile()
        block = slots.at[which, pl.ds(0, len(EVERY))]
        total = pltpu.make_async_remote_copy(src_ref=block, dst_ref=block, send_sem=sum_send.at[which], recv_sem=sum_recv.at[which], device_id=partner, device_id_type=MESH)
        total.wait_recv()
        sum_sent.append(total)
        received = [slots[which, slot] for slot in range(DEVICES)]
        while len(received) > 1:
            received = [left + right for left, right in zip(received[::2], received[1::2])]
        return received[0]

    grad_sq = global_sum(0, jnp.sum(fold(columns_loop(gather_sum, zero)), axis=0, keepdims=True))
    norm_sq = jnp.sum(grad_sq, axis=1, keepdims=True) / (REPLICAS * REPLICAS)
    clip = jnp.minimum(1.0, MAX_NORM / jnp.sqrt(norm_sq)) / REPLICAS

    def new_moments(tile, cols):
        scaled = clip * grad_sum[tile, :, cols]
        new_one = BETA_ONE * one[tile, :, cols] + (1.0 - BETA_ONE) * scaled
        new_two = BETA_TWO * two[tile, :, cols] + (1.0 - BETA_TWO) * scaled * scaled
        return new_one, new_two

    def moments(offset, carry):
        squares = []
        for tile in range(TILES):
            new_one, new_two = new_moments(tile, at(offset))
            step = (new_one * (1.0 / CORR_ONE)) / (jnp.sqrt(new_two * (1.0 / CORR_TWO)) + EPSILON) + WEIGHT_DECAY * master[tile, :, at(offset)]
            direction[tile, :, at(offset)] = step
            squares.append(carry[tile] + step * step)
        return tuple(squares)

    def store_moments():
        for side in (0, 1):
            remote(part(direction, side), part(ahead_step.at[side], side), ring_b(side), 'step', ahead_sem.at[1])

        def body(offset, carry):
            for tile in range(TILES):
                one_out[tile, :, at(offset)], two_out[tile, :, at(offset)] = new_moments(tile, at(offset))
            return carry
        columns_loop(body)

    step_sq = [jnp.sum(fold(value), axis=1, keepdims=True) for value in columns_loop(moments, (zero,) * TILES)]

    lane = lax.broadcasted_iota(jnp.int32, (8, 128), 1)
    sub = lax.broadcasted_iota(jnp.int32, (8, 128), 0)
    spread_sums = jnp.zeros((8, 128), jnp.float32)
    for tile in range(TILES):
        spread_sums = jnp.where(lane == 8 * tile + sub, step_sq[tile], spread_sums)
        spread_sums = jnp.where(lane == 32 + 8 * tile + sub, weight_sq[tile], spread_sums)

    def tensor_of(row):
        layer = jnp.where(row >= 12, 1, 0)
        block = row - 12 * layer
        return 4 * layer + jnp.where(block >= 3, 1, 0) + jnp.where(block >= 4, 1, 0) + jnp.where(block >= 8, 1, 0)

    masks = []
    for tile in range(TILES):
        tensor = tensor_of(8 * tile + sub)
        masks.append(((tensor_of(lane) == tensor) & (lane < 24), (tensor_of(lane - 32) == tensor) & (lane >= 32) & (lane < 56)))
    row_sums = jnp.broadcast_to(global_sum(1, jnp.sum(spread_sums, axis=0, keepdims=True), store_moments), (8, 128))
    rate = []
    for step_mask, weight_mask in masks:
        step_norm, weight_norm = (jnp.sqrt(jnp.sum(jnp.where(mask, row_sums, 0.0), axis=1, keepdims=True)) for mask in (step_mask, weight_mask))
        rate.append(LEARN_RATE * (weight_norm / step_norm))

    def weights(db, weight, step, master_new=None, first=0, length=SLAB):
        start = column(0, db)

        def body(offset, carry):
            for tile in range(TILES):
                value = weight[tile, :, at(first + offset)] - rate[tile] * step[tile, :, at(first + offset)]
                if master_new is not None:
                    master_new[tile, :, at(first + offset)] = value
                params[tile, :, at(start + first + offset)] = value.astype(jnp.bfloat16)
            return carry

        columns_loop(body, 0, length)

    handed = []
    along_a = {}
    far_b = {}
    far_a = {}

    def send(da, db, half, device):
        ref = piece(params, da, db, half)
        return remote(ref, ref, device)

    def give(ref, device):
        handed.append(ref.shape[-1])
        remote(ref, ref, device, 'gather', hand_sem)

    def hand(da, db, half):
        give(piece(params, da, db, half), partner)

    def pass_on(first, second):
        for one_piece, other_piece in ((first, second), (second, first)):
            along_a[0, one_piece] = send(0, *one_piece, ring_a(0))
            along_a[1, other_piece] = send(0, *other_piece, ring_a(1))

    def quarter(da, half, index):
        start = column(da, 2) + half * HALF + index * QUARTER
        return params.at[:, :, pl.ds(pl.multiple_of(start, QUARTER), QUARTER)]

    def arrived(side, db, half):
        along_a[side, (db, half)].wait_recv()
        da = 3 - 2 * side
        if half == side and db == 2:
            first, second = quarter(da, half, 0), quarter(da, half, 1)
            far_a[db, half] = remote(first, first, ring_a(side))
            give(second, ring_a(side))
            give(second, peer(0, (1 - 2 * side) * core, (1 - 2 * side) * (1 - core), 1))
        elif half == side:
            far_a[db, half] = send(da, db, half, ring_a(side))
        hand(da, db, half)

    for half in (0, 1):
        weights(0, master, direction, master_out, half * HALF, HALF)
        along_a[half, (0, half)] = send(0, 0, half, ring_a(half))
    for side in (0, 1):
        along_a[side, (0, 1 - side)] = send(0, 0, 1 - side, ring_a(side))
    hand(0, 0, 0)
    hand(0, 0, 1)
    along_b = [send(0, 0, 1 - side, ring_b(side)) for side in (0, 1)]
    all_of(ahead_weight.at[0], 'weight', ahead_sem.at[0]).wait_recv()
    all_of(ahead_step.at[0], 'step', ahead_sem.at[1]).wait_recv()
    for side in (0, 1):
        db = 3 - 2 * side
        weights(db, ahead_weight.at[side], ahead_step.at[side], None, side * HALF, HALF)
        far_b[side] = send(0, db, side, ring_b(side))
    pass_on((3, 0), (1, 1))
    hand(0, 3, 0)
    hand(0, 1, 1)
    for side in (0, 1):
        arrived(side, 0, side)
    for side in (0, 1):
        along_b[side].wait_recv()
    pass_on((1, 0), (3, 1))
    hand(0, 1, 0)
    hand(0, 3, 1)
    for side in (0, 1):
        far_b[side].wait_recv()
    pass_on((2, 0), (2, 1))
    hand(0, 2, 0)
    hand(0, 2, 1)
    for ref, group in ((relay_raw, 'raw'), (pair_raw, 'pair'), (early, 'early'), (late, 'late'), (mid, 'mid'), (end, 'end'), (ahead_weight.at[0], 'weight'), (ahead_step.at[0], 'step')):
        all_of(ref, group).wait_send()
    for copy in sum_sent:
        copy.wait_send()
    for side in (0, 1):
        arrived(side, 0, 1 - side)
    for pieces in (((3, 0), (1, 1)), ((1, 1), (3, 0)), ((1, 0), (3, 1)), ((3, 1), (1, 0)), ((2, 0), (2, 1)), ((2, 1), (2, 0))):
        for side in (0, 1):
            arrived(side, *pieces[side])
    for db in (0, 3, 1, 2):
        for half in (0, 1):
            far_a[db, half].wait_recv()
            if db == 2:
                give(quarter(2, half, 0), partner)
            else:
                hand(2, db, half)
    if len(started) != COPIES:
        raise ValueError(len(started))
    all_of(params.at[:, :, pl.ds(0, sum(handed))], landing=hand_sem).wait_recv()
    all_of(params.at[:, :, pl.ds(0, sum(gathered))]).wait_send()


def write_kernel(params, master, one, two, params_out, master_out, one_out, two_out, sem):
    pairs = [(master, master_out), (one, one_out), (two, two_out)]
    width = params.shape[2] // WRITE_PIECES
    for tile in range(TILES):
        for index in range(WRITE_PIECES):
            cols = pl.ds(index * width, width)
            pltpu.make_async_copy(params.at[tile, :, cols], params_out.at[tile, :, cols], sem.at[0]).start()
    copies = [pltpu.make_async_copy(src, dst, sem.at[1 + index]) for index, (src, dst) in enumerate(pairs)]
    for copy in copies:
        copy.start()
    for copy in copies:
        copy.wait()
    pltpu.make_async_copy(params, params_out, sem.at[0]).wait()


def solution(mesh):
    state_spec = P(None, ('model', 'data'))

    def device_step(local_grads, master, moment_one, moment_two):
        state = (TILES, 8, SLAB)
        width = local_grads.shape[2]
        hbm = pl.BlockSpec(memory_space=pltpu.HBM)
        vmem = pl.BlockSpec(memory_space=pltpu.VMEM)

        def slabs(count, dtype, length=SLAB):
            return pltpu.VMEM(count + (TILES, 8, length), dtype)

        operands = (local_grads.reshape(TILES, 8, width), master.reshape(state), moment_one.reshape(state), moment_two.reshape(state))
        results = pl.pallas_call(
            lamb_kernel,
            name='lamb_step',
            out_shape=(
                pltpu.VMEM((TILES, 8, width), jnp.bfloat16),
                pltpu.VMEM(state, jnp.float32),
                pltpu.VMEM(state, jnp.float32),
                pltpu.VMEM(state, jnp.float32),
            ),
            in_specs=[hbm] * 4,
            out_specs=(vmem,) * 4,
            scratch_shapes=[
                slabs((len(ORDER),), jnp.bfloat16),
                slabs((len(ORDER),), jnp.bfloat16),
                slabs((2, 2, PIECES), jnp.bfloat16, HALF),
                slabs((2, PIECES), jnp.float32, HALF),
                slabs((2, PIECES), jnp.float32, HALF),
                slabs((2, 4), jnp.float32),
                slabs((4,), jnp.float32),
                slabs((2,), jnp.float32, HALF),
                slabs((2,), jnp.float32),
                slabs((3,), jnp.float32),
                slabs((), jnp.float32),
                slabs((), jnp.float32),
                slabs((2,), jnp.float32),
                slabs((2,), jnp.float32),
                pltpu.VMEM((2, 1, 128), jnp.float32),
                pltpu.VMEM((2, DEVICES, 1, 128), jnp.float32),
                pltpu.SemaphoreType.DMA((len(GROUPS),)),
                pltpu.SemaphoreType.DMA((COPIES,)),
                pltpu.SemaphoreType.DMA((2,)),
                pltpu.SemaphoreType.DMA((2,)),
                pltpu.SemaphoreType.DMA((5,)),
                pltpu.SemaphoreType.DMA((2, PIECES)),
                pltpu.SemaphoreType.DMA((len(ORDER) // BATCH,)),
                pltpu.SemaphoreType.DMA((2,)),
                pltpu.SemaphoreType.REGULAR((len(STAGES),)),
            ],
            compiler_params=pltpu.CompilerParams(collective_id=0, has_side_effects=True, vmem_limit_bytes=VMEM_LIMIT),
        )(*(pltpu.with_memory_space_constraint(operand, pltpu.HBM) for operand in operands))
        outs = pl.pallas_call(
            write_kernel,
            name='write_out',
            out_shape=tuple(pltpu.HBM(result.shape, result.dtype) for result in results),
            in_specs=[vmem] * 4,
            out_specs=(hbm,) * 4,
            scratch_shapes=[pltpu.SemaphoreType.DMA((4,))],
            compiler_params=pltpu.CompilerParams(vmem_limit_bytes=2 ** 20),
        )(*results)
        return tuple(out.reshape(24, -1) for out in outs)

    return jax.shard_map(device_step, mesh=mesh, in_specs=(P('data', None, 'model'), state_spec, state_spec, state_spec), out_specs=(P(None, 'model'), state_spec, state_spec, state_spec), check_vma=False)
```
